8 devices in a mesh: prob: 1 (over z), row: 2 (over y), col: 4 (over x, core).
Axes of the slice: x: 2, y: 2, z: 1, core: 2. Of those that a mesh axis runs over, the one named last changes fastest.
Arguments:
- kernel: bfloat16 [2048, 16384], P('row', 'col')
- cost_mat: bfloat16 [2048, 16384], P('row', 'col')
- src_mass: float32 [2048, 32], P('row', 'prob')
- tgt_mass: float32 [16384, 32], P('col', 'prob')
Outputs:
- output 1: float32 [2048, 32], P('row', 'prob')
- output 2: float32 [16384, 32], P('col', 'prob')
- output 3: float32 [32], P('prob')
All inputs are finite; a program needn't handle non-finite values.
Results may differ from the reference program's by a relative error of at most 0.001.
Values are sent between devices in bfloat16 or wider.
A program may use at most 1 GiB of HBM per device.

```python
import jax
import jax.numpy as jnp
from jax import lax

N_SRC = 2048
N_TGT = 16384
BATCH = 32
SWEEPS = 6
EPSILON = 0.1


def setup_inputs(seed: int = 0, part: int = 0) -> dict:
    base_key = jax.random.key(seed)
    key_src, key_tgt = jax.random.split(base_key, 2)
    src_pts = jax.random.uniform(key_src, (N_SRC, 3), jnp.float32)
    tgt_pts = jax.random.uniform(key_tgt, (N_TGT, 3), jnp.float32)
    cross_dot = jnp.dot(src_pts, tgt_pts.T)
    dist_sq = jnp.sum(src_pts * src_pts, axis=1)[:, None] + jnp.sum(tgt_pts * tgt_pts, axis=1)[None, :] - 2.0 * cross_dot
    cost_full = jnp.clip(dist_sq / 3.0, 0.0, 1.0)
    part_key = jax.random.fold_in(jax.random.key(seed + 1), part)
    key_a, key_b = jax.random.split(part_key, 2)
    src_mass = N_TGT * jax.random.uniform(key_a, (N_SRC, BATCH), jnp.float32, 0.25, 1.75)
    tgt_mass = N_SRC * jax.random.uniform(key_b, (N_TGT, BATCH), jnp.float32, 0.25, 1.75)
    return {"kernel": jnp.exp(-cost_full / EPSILON).astype(jnp.bfloat16), "cost_mat": cost_full.astype(jnp.bfloat16), "src_mass": src_mass, "tgt_mass": tgt_mass}


def reference(kernel, cost_mat, src_mass, tgt_mass):
    def sweep(carry, unused):
        tgt_scale = carry[1]
        row_sum = jnp.dot(kernel, tgt_scale.astype(jnp.bfloat16), preferred_element_type=jnp.float32)
        src_scale = src_mass / row_sum
        col_sum = lax.dot_general(kernel, src_scale.astype(jnp.bfloat16), (((0,), (0,)), ((), ())), preferred_element_type=jnp.float32)
        return (src_scale, tgt_mass / col_sum), None
    start = (jnp.zeros((N_SRC, BATCH), jnp.float32), jnp.ones((N_TGT, BATCH), jnp.float32))
    final, unused_hist = lax.scan(sweep, start, None, length=SWEEPS)
    src_scale, tgt_scale = final
    kern_cost = kernel * cost_mat
    weighted = jnp.dot(kern_cost, tgt_scale.astype(jnp.bfloat16), preferred_element_type=jnp.float32)
    transport = jnp.sum(src_scale * weighted, axis=0) / (N_SRC * N_TGT)
    return (src_scale, tgt_scale, transport)
```

```python
import functools

import jax
import jax.numpy as jnp
from jax import lax
from jax.experimental import pallas as pl
from jax.experimental.pallas import tpu as pltpu
from jax.sharding import PartitionSpec as P

SWEEPS = 6
HALF_CHUNKS = 4
MESH = pl.DeviceIdType.MESH
F32 = jnp.float32
BF16 = jnp.bfloat16


def _dot_t(lhs, rhs):
    return lax.dot_general(lhs, rhs, (((1,), (1,)), ((), ())), preferred_element_type=F32)


def _kernel(norm, kern_hbm, cost_hbm, src_hbm, tgt_hbm, u_hbm, v_hbm, out_hbm,
            kern, cost, src, tgt, u_half, s_acc, s_out, s_in, x_out, x_in,
            t_out, t_own, t_in, v_out, v_in, t_full, v_full, w_acc, c_all, c_out,
            load_sem, tgt_sem, src_sem, store_sem, bar_dummy,
            sd_send, sd_recv, ud_send, ud_recv, sx_send, sx_recv,
            ty_send, ty_recv, vy_send, vy_recv, tf_send, tf_recv, c_send, c_recv):
    row = lax.axis_index("row")
    col = lax.axis_index("col")
    core = lax.rem(col, 2)
    chip = col // 2
    other_core = 1 - core
    other_row = 1 - row
    mate = {"col": chip * 2 + other_core}
    across = {"col": (1 - chip) * 2 + core}
    above = {"row": other_row}
    n_chunk, rows, width = kern.shape
    half = n_chunk // 2
    mid = rows // 2

    def load(hbm, buf, i):
        return pltpu.make_async_copy(hbm.at[:, pl.ds(i * width, width)], buf.at[i], load_sem.at[i])

    for i in range(n_chunk):
        load(kern_hbm, kern, i).start()
    src_copy = pltpu.make_async_copy(src_hbm.at[:, pl.ds(pl.multiple_of(core * mid, mid), mid)], src, src_sem)
    src_copy.start()
    for i in range(n_chunk):
        pltpu.make_async_copy(tgt_hbm.at[:, pl.ds(i * width, width)], tgt.at[i], tgt_sem.at[i]).start()

    barrier = pltpu.get_barrier_semaphore()
    me = row * 4 + col
    for d in range(1, 8):
        peer = lax.rem(me + d, 8)
        pl.semaphore_signal(barrier, inc=1, device_id={"row": peer // 4, "col": lax.rem(peer, 4)}, device_id_type=MESH)
    pl.semaphore_wait(barrier, 7)

    def remote(src_ref, dst_ref, send, recv, dev):
        return pltpu.make_async_remote_copy(src_ref=src_ref, dst_ref=dst_ref, send_sem=send, recv_sem=recv,
                                            device_id=dev, device_id_type=MESH)

    def reduce_rows(parity):
        s_out[0] = s_acc[:, 0:mid]
        s_out[1] = s_acc[:, mid:rows]
        to_mate = remote(s_out.at[other_core], s_in, sd_send, sd_recv, mate)
        to_mate.start()
        to_mate.wait_recv()
        chip_sum = s_out[core] + s_in[...]
        x_out[...] = chip_sum
        to_across = remote(x_out, x_in.at[parity], sx_send.at[parity], sx_recv.at[parity], across)
        to_across.start()
        to_across.wait_recv()
        u_half[core] = src[...] / (x_out[...] + x_in[parity])
        share = remote(u_half.at[core], u_half.at[core], ud_send, ud_recv, mate)
        share.start()
        to_mate.wait_send()
        to_across.wait_send()
        share.wait()

    def scaled_cols(u_lo, u_hi, i):
        return (jnp.dot(u_lo, kern[i, 0:mid, :], preferred_element_type=F32)
                + jnp.dot(u_hi, kern[i, mid:rows, :], preferred_element_type=F32))

    ones = jnp.ones((32, width), BF16)
    for i in range(n_chunk):
        load(kern_hbm, kern, i).wait()
        part = _dot_t(ones, kern[i])
        if i == 0:
            s_acc[...] = part
        else:
            s_acc[...] += part
    for i in range(n_chunk):
        load(cost_hbm, cost, i).start()
    src_copy.wait()
    for i in range(n_chunk):
        pltpu.make_async_copy(tgt_hbm.at[:, pl.ds(i * width, width)], tgt.at[i], tgt_sem.at[i]).wait()
    reduce_rows(0)

    def sweep(step, carry):
        u_lo = u_half[0].astype(BF16)
        u_hi = u_half[1].astype(BF16)
        sends = []
        for i in range(half):
            t_out[i] = scaled_cols(u_lo, u_hi, other_row * half + i)
            copy = remote(t_out.at[i], t_in.at[i], ty_send.at[i], ty_recv.at[i], above)
            copy.start()
            sends.append(copy)
        for i in range(half):
            t_own[i] = scaled_cols(u_lo, u_hi, row * half + i)
        shares = []
        for i in range(half):
            sends[i].wait_recv()
            v = tgt[row * half + i] / (t_own[i] + t_in[i])
            vb = v.astype(BF16)
            v_out[i] = vb
            copy = remote(v_out.at[i], v_in.at[i], vy_send.at[i], vy_recv.at[i], above)
            copy.start()
            shares.append(copy)
            part = _dot_t(vb, kern[row * half + i])
            if i == 0:
                s_acc[...] = part
            else:
                s_acc[...] += part
        for i in range(half):
            shares[i].wait_recv()
            s_acc[...] += _dot_t(v_in[i], kern[other_row * half + i])
        for i in range(half):
            sends[i].wait_send()
            shares[i].wait_send()
        reduce_rows(lax.rem(step + 1, 2))
        return carry

    lax.fori_loop(0, SWEEPS - 1, sweep, 0)

    u_lo = u_half[0].astype(BF16)
    u_hi = u_half[1].astype(BF16)
    lasts = []
    for i in range(n_chunk):
        t_full[i] = scaled_cols(u_lo, u_hi, i)
        copy = remote(t_full.at[i], v_full.at[i], tf_send.at[i], tf_recv.at[i], above)
        copy.start()
        lasts.append(copy)
    u_stores = [pltpu.make_async_copy(u_half.at[j], u_hbm.at[:, pl.ds(j * mid, mid)], store_sem.at[n_chunk + j]) for j in range(2)]
    for copy in u_stores:
        copy.start()
    for i in range(n_chunk):
        load(cost_hbm, cost, i).wait()
        cost[i] = kern[i] * cost[i]
    stores = []
    for i in range(n_chunk):
        lasts[i].wait_recv()
        v = tgt[i] / (t_full[i] + v_full[i])
        tgt[i] = v
        copy = pltpu.make_async_copy(tgt.at[i], v_hbm.at[:, pl.ds(i * width, width)], store_sem.at[i])
        copy.start()
        stores.append(copy)
        part = _dot_t(v.astype(BF16), cost[i])
        if i == 0:
            w_acc[...] = part
        else:
            w_acc[...] += part
    total = jnp.sum(u_half[0] * w_acc[:, 0:mid] + u_half[1] * w_acc[:, mid:rows], axis=1, keepdims=True)
    c_all[me] = jnp.broadcast_to(total, (32, 128))
    pieces = []
    for d in range(1, 8):
        peer = lax.rem(me + d, 8)
        copy = remote(c_all.at[me], c_all.at[me], c_send.at[d - 1], c_recv.at[d - 1],
                      {"row": peer // 4, "col": lax.rem(peer, 4)})
        copy.start()
        pieces.append(copy)
    for copy in lasts:
        copy.wait_send()
    for copy in pieces:
        copy.wait()
    grand = c_all[0]
    for j in range(1, 8):
        grand = grand + c_all[j]
    c_out[...] = grand / norm
    last = pltpu.make_async_copy(c_out, out_hbm, bar_dummy)
    last.start()
    for copy in u_stores + stores:
        copy.wait()
    last.wait()


def solution(mesh):
    row_size = mesh.shape["row"]
    col_size = mesh.shape["col"]

    def local_fn(kernel, cost_mat, src_mass, tgt_mass):
        rows, cols = kernel.shape
        q = src_mass.shape[1]
        n_chunk = 2 * HALF_CHUNKS
        width = cols // n_chunk
        mid = rows // 2
        norm = float(rows * row_size * cols * col_size)
        dma = pltpu.SemaphoreType.DMA
        anyspace = pl.BlockSpec(memory_space=pl.ANY)
        scratch = [
            pltpu.VMEM((n_chunk, rows, width), BF16),
            pltpu.VMEM((n_chunk, rows, width), BF16),
            pltpu.VMEM((q, mid), F32),
            pltpu.VMEM((n_chunk, q, width), F32),
            pltpu.VMEM((2, q, mid), F32),
            pltpu.VMEM((q, rows), F32),
            pltpu.VMEM((2, q, mid), F32),
            pltpu.VMEM((q, mid), F32),
            pltpu.VMEM((q, mid), F32),
            pltpu.VMEM((2, q, mid), F32),
            pltpu.VMEM((HALF_CHUNKS, q, width), F32),
            pltpu.VMEM((HALF_CHUNKS, q, width), F32),
            pltpu.VMEM((HALF_CHUNKS, q, width), F32),
            pltpu.VMEM((HALF_CHUNKS, q, width), BF16),
            pltpu.VMEM((HALF_CHUNKS, q, width), BF16),
            pltpu.VMEM((n_chunk, q, width), F32),
            pltpu.VMEM((n_chunk, q, width), F32),
            pltpu.VMEM((q, rows), F32),
            pltpu.VMEM((8, q, 128), F32),
            pltpu.VMEM((q, 128), F32),
            dma((n_chunk,)), dma((n_chunk,)), dma, dma((n_chunk + 2,)), dma,
            dma, dma, dma, dma, dma((2,)), dma((2,)),
            dma((HALF_CHUNKS,)), dma((HALF_CHUNKS,)), dma((HALF_CHUNKS,)), dma((HALF_CHUNKS,)),
            dma((n_chunk,)), dma((n_chunk,)), dma((7,)), dma((7,)),
        ]
        u_t, v_t, cost = pl.pallas_call(
            functools.partial(_kernel, norm),
            out_shape=(
                jax.ShapeDtypeStruct((q, rows), F32),
                jax.ShapeDtypeStruct((q, cols), F32),
                jax.ShapeDtypeStruct((q, 128), F32),
            ),
            in_specs=[anyspace] * 4,
            out_specs=(anyspace,) * 3,
            scratch_shapes=scratch,
            compiler_params=pltpu.CompilerParams(collective_id=0, has_side_effects=True, vmem_limit_bytes=48 * 1024 * 1024),
            name="sinkhorn",
        )(kernel, cost_mat, src_mass.T, tgt_mass.T)
        return u_t.T, v_t.T, cost[:, 0]

    return jax.shard_map(local_fn, mesh=mesh, in_specs=(P("row", "col"), P("row", "col"), P("row", "prob"), P("col", "prob")), out_specs=(P("row", "prob"), P("col", "prob"), P("prob")), check_vma=False)
```

```python
import functools

import jax
import jax.numpy as jnp
from jax import lax
from jax.experimental import pallas as pl
from jax.experimental.pallas import tpu as pltpu
from jax.sharding import PartitionSpec as P

SWEEPS = 6
CHUNKS = 8
EARLY = 5
GROUPS = 2
MESH = pl.DeviceIdType.MESH
F32 = jnp.float32
BF16 = jnp.bfloat16


def _dot_t(lhs, rhs):
    return lax.dot_general(lhs, rhs, (((1,), (1,)), ((), ())), preferred_element_type=F32)


def _kernel(norm, kern_hbm, cost_hbm, src_hbm, tgt_hbm, u_hbm, v_hbm, out_hbm,
            kern, cost, src, tgt, u_all, s_acc, s_in, x_out, x_in, t_out, t_in, v_all, w_acc, c_all, c_out,
            load_sem, tgt_sem, src_sem, v_sem, u_sem, out_sem,
            s_send, s_recv, x_send, x_recv, t_send, t_recv, c_send, c_recv):
    row = lax.axis_index("row")
    col = lax.axis_index("col")
    core = lax.rem(col, 2)
    chip = col // 2
    mate = {"col": chip * 2 + (1 - core)}
    across = {"col": (1 - chip) * 2 + (1 - core)}
    above = {"row": 1 - row}
    n_chunk, rows, width = kern.shape
    q = t_out.shape[2]
    me = row * 4 + col

    def load(hbm, buf, i):
        return pltpu.make_async_copy(hbm.at[:, pl.ds(i * width, width)], buf.at[i], load_sem.at[i])

    def load_tgt(i):
        return pltpu.make_async_copy(tgt_hbm.at[:, pl.ds(i * width, width)], tgt.at[i], tgt_sem.at[i])

    for i in range(n_chunk):
        load(kern_hbm, kern, i).start()
    src_copy = pltpu.make_async_copy(src_hbm, src, src_sem)
    src_copy.start()
    for i in range(n_chunk):
        load_tgt(i).start()

    barrier = pltpu.get_barrier_semaphore()
    for d in range(1, 8):
        peer = lax.rem(me + d, 8)
        pl.semaphore_signal(barrier, inc=1, device_id={"row": peer // 4, "col": lax.rem(peer, 4)}, device_id_type=MESH)
    pl.semaphore_wait(barrier, 7)

    def remote(src_ref, dst_ref, send, recv, dev):
        return pltpu.make_async_remote_copy(src_ref=src_ref, dst_ref=dst_ref, send_sem=send, recv_sem=recv,
                                            device_id=dev, device_id_type=MESH)

    def pair_copy(g, p):
        return remote(s_acc.at[g], s_in.at[g, p], s_send.at[g], s_recv.at[g, p], mate)

    def chip_copy(g, p):
        return remote(x_out.at[g], x_in.at[g, p], x_send.at[g], x_recv.at[g, p], across)

    def row_copy(g, p, i):
        return remote(t_out.at[g, i], t_in.at[g, p, i], t_send.at[g, i], t_recv.at[g, p, i], above)

    def relay(g, p):
        pair_copy(g, p).wait_recv()
        x_out[g] = s_acc[g] + s_in[g, p]
        chip_copy(g, p).start()

    def finish(g, p, groups):
        chip_copy(g, p).wait_recv()
        total = x_out[g] + x_in[g, p]
        for h in groups:
            u_all[h] = src[h * q:(h + 1) * q] / total
        pair_copy(g, p).wait_send()
        chip_copy(g, p).wait_send()

    def send_cols(g, p):
        u = u_all[g].astype(BF16)
        for i in range(n_chunk):
            t_out[g, i] = jnp.dot(u, kern[i], preferred_element_type=F32)
            row_copy(g, p, i).start()

    def new_scale(g, p, i):
        row_copy(g, p, i).wait_recv()
        return tgt[i, g * q:(g + 1) * q] / (t_out[g, i] + t_in[g, p, i])

    def take_cols(g, p, lo, hi):
        for i in range(lo, hi):
            part = _dot_t(new_scale(g, p, i).astype(BF16), kern[i])
            if i == 0:
                s_acc[g] = part
            else:
                s_acc[g] += part
        if hi == n_chunk:
            pair_copy(g, 1 - p).start()
            for i in range(n_chunk):
                row_copy(g, p, i).wait_send()

    def take_last(g, p):
        for i in range(n_chunk):
            v = new_scale(g, p, i)
            v_all[i, g * q:(g + 1) * q] = v
            store_v(g, i).start()
            part = _dot_t(v.astype(BF16), cost[i])
            if i == 0:
                w_acc[g] = part
            else:
                w_acc[g] += part
        for i in range(n_chunk):
            row_copy(g, p, i).wait_send()
        c_all[me, g * q:(g + 1) * q] = jnp.broadcast_to(jnp.sum(u_all[g] * w_acc[g], axis=1, keepdims=True), (q, 128))

    def store_v(g, i):
        return pltpu.make_async_copy(v_all.at[i, pl.ds(g * q, q)], v_hbm.at[pl.ds(g * q, q), pl.ds(i * width, width)], v_sem.at[g, i])

    def store_u(g):
        return pltpu.make_async_copy(u_all.at[g], u_hbm.at[pl.ds(g * q, q)], u_sem.at[g])

    ones = jnp.ones((q, width), BF16)
    for i in range(n_chunk):
        load(kern_hbm, kern, i).wait()
        part = _dot_t(ones, kern[i])
        if i == 0:
            s_acc[0] = part
        else:
            s_acc[0] += part
    pair_copy(0, 0).start()
    for i in range(n_chunk):
        load(cost_hbm, cost, i).start()
    src_copy.wait()
    for i in range(n_chunk):
        load_tgt(i).wait()
    relay(0, 0)
    finish(0, 0, range(GROUPS))

    send_cols(0, 0)
    send_cols(1, 0)
    take_cols(0, 0, 0, n_chunk)
    relay(0, 1)
    take_cols(1, 0, 0, EARLY)
    finish(0, 1, (0,))

    def sweep(step, carry):
        p = lax.rem(step, 2)
        send_cols(0, p)
        take_cols(1, 1 - p, EARLY, n_chunk)
        relay(1, p)
        take_cols(0, p, 0, EARLY)
        finish(1, p, (1,))
        send_cols(1, p)
        take_cols(0, p, EARLY, n_chunk)
        relay(0, 1 - p)
        take_cols(1, p, 0, EARLY)
        finish(0, 1 - p, (0,))
        return carry

    lax.fori_loop(1, SWEEPS - 1, sweep, 0)

    p = (SWEEPS - 1) % 2
    send_cols(0, p)
    store_u(0).start()
    take_cols(1, 1 - p, EARLY, n_chunk)
    relay(1, p)
    for i in range(n_chunk):
        load(cost_hbm, cost, i).wait()
        cost[i] = kern[i] * cost[i]
    finish(1, p, (1,))
    send_cols(1, p)
    store_u(1).start()
    take_last(0, p)
    take_last(1, p)

    def share(d):
        peer = lax.rem(me + d, 8)
        return remote(c_all.at[me], c_all.at[me], c_send.at[d - 1], c_recv.at[d - 1],
                      {"row": peer // 4, "col": lax.rem(peer, 4)})

    for d in range(1, 8):
        share(d).start()
    for d in range(1, 8):
        share(d).wait()
    grand = c_all[0]
    for j in range(1, 8):
        grand = grand + c_all[j]
    c_out[...] = grand / norm
    last = pltpu.make_async_copy(c_out, out_hbm, out_sem)
    last.start()
    for g in range(GROUPS):
        store_u(g).wait()
        for i in range(n_chunk):
            store_v(g, i).wait()
    last.wait()


def solution(mesh):
    row_size = mesh.shape["row"]
    col_size = mesh.shape["col"]

    def local_fn(kernel, cost_mat, src_mass, tgt_mass):
        rows, cols = kernel.shape
        batch = src_mass.shape[1]
        q = batch // GROUPS
        width = cols // CHUNKS
        norm = float(rows * row_size * cols * col_size)
        dma = pltpu.SemaphoreType.DMA
        anyspace = pl.BlockSpec(memory_space=pl.ANY)
        scratch = [
            pltpu.VMEM((CHUNKS, rows, width), BF16),
            pltpu.VMEM((CHUNKS, rows, width), BF16),
            pltpu.VMEM((batch, rows), F32),
            pltpu.VMEM((CHUNKS, batch, width), F32),
            pltpu.VMEM((GROUPS, q, rows), F32),
            pltpu.VMEM((GROUPS, q, rows), F32),
            pltpu.VMEM((GROUPS, 2, q, rows), F32),
            pltpu.VMEM((GROUPS, q, rows), F32),
            pltpu.VMEM((GROUPS, 2, q, rows), F32),
            pltpu.VMEM((GROUPS, CHUNKS, q, width), F32),
            pltpu.VMEM((GROUPS, 2, CHUNKS, q, width), F32),
            pltpu.VMEM((CHUNKS, batch, width), F32),
            pltpu.VMEM((GROUPS, q, rows), F32),
            pltpu.VMEM((8, batch, 128), F32),
            pltpu.VMEM((batch, 128), F32),
            dma((CHUNKS,)), dma((CHUNKS,)), dma, dma((GROUPS, CHUNKS)), dma((GROUPS,)), dma,
            dma((GROUPS,)), dma((GROUPS, 2)), dma((GROUPS,)), dma((GROUPS, 2)),
            dma((GROUPS, CHUNKS)), dma((GROUPS, 2, CHUNKS)), dma((7,)), dma((7,)),
        ]
        u_t, v_t, cost = pl.pallas_call(
            functools.partial(_kernel, norm),
            out_shape=(
                jax.ShapeDtypeStruct((batch, rows), F32),
                jax.ShapeDtypeStruct((batch, cols), F32),
                jax.ShapeDtypeStruct((batch, 128), F32),
            ),
            in_specs=[anyspace] * 4,
            out_specs=(anyspace,) * 3,
            scratch_shapes=scratch,
            compiler_params=pltpu.CompilerParams(collective_id=0, has_side_effects=True, vmem_limit_bytes=48 * 1024 * 1024),
            name="sinkhorn",
        )(kernel, cost_mat, src_mass.T, tgt_mass.T)
        return u_t.T, v_t.T, cost[:, 0]

    return jax.shard_map(local_fn, mesh=mesh, in_specs=(P("row", "col"), P("row", "col"), P("row", "prob"), P("col", "prob")), out_specs=(P("row", "prob"), P("col", "prob"), P("prob")), check_vma=False)
```

```python
import functools

import jax
import jax.numpy as jnp
from jax import lax
from jax.experimental import pallas as pl
from jax.experimental.pallas import tpu as pltpu
from jax.sharding import PartitionSpec as P

SWEEPS = 6
CHUNKS = 8
EARLY = 5
GROUPS = 2
MESH = pl.DeviceIdType.MESH
F32 = jnp.float32
BF16 = jnp.bfloat16


def _dot_t(lhs, rhs):
    return lax.dot_general(lhs, rhs, (((1,), (1,)), ((), ())), preferred_element_type=F32)


def _emit(u_ref, v_ref, c_ref, u_hbm, v_hbm, c_out, sems):
    copies = [pltpu.make_async_copy(u_ref, u_hbm, sems.at[0]), pltpu.make_async_copy(v_ref, v_hbm, sems.at[1])]
    for copy in copies:
        copy.start()
    c_out[...] = c_ref[0, 0:c_out.shape[0]]
    for copy in copies:
        copy.wait()


def _kernel(norm, kern_hbm, cost_hbm, src_hbm, tgt_hbm, u_out, v_out, c_out,
            kern, kern_t, cost, src, tgt, u_all, s_acc, s_in, x_out, x_in, t_out, t_in, w_acc, c_all, z_all,
            load_sem, tgt_sem, src_sem,
            s_send, s_recv, x_send, x_recv, t_send, t_recv, c_send, c_recv, z_send, z_recv):
    row = lax.axis_index("row")
    col = lax.axis_index("col")
    core = lax.rem(col, 2)
    chip = col // 2
    mate = {"col": chip * 2 + (1 - core)}
    across = {"col": (1 - chip) * 2 + (1 - core)}
    above = {"row": 1 - row}
    n_chunk, rows, width = kern.shape
    q = t_out.shape[2]
    me = row * 4 + col

    def load(hbm, buf, i):
        return pltpu.make_async_copy(hbm.at[:, pl.ds(i * width, width)], buf.at[i], load_sem.at[i])

    def load_tgt(i):
        return pltpu.make_async_copy(tgt_hbm.at[:, pl.ds(i * width, width)], tgt.at[i], tgt_sem.at[i])

    for i in range(n_chunk):
        load(kern_hbm, kern, i).start()
    src_copy = pltpu.make_async_copy(src_hbm, src, src_sem)
    src_copy.start()
    for i in range(n_chunk):
        load_tgt(i).start()

    barrier = pltpu.get_barrier_semaphore()
    for d in range(1, 8):
        peer = lax.rem(me + d, 8)
        pl.semaphore_signal(barrier, inc=1, device_id={"row": peer // 4, "col": lax.rem(peer, 4)}, device_id_type=MESH)
    pl.semaphore_wait(barrier, 7)

    def remote(src_ref, dst_ref, send, recv, dev):
        return pltpu.make_async_remote_copy(src_ref=src_ref, dst_ref=dst_ref, send_sem=send, recv_sem=recv,
                                            device_id=dev, device_id_type=MESH)

    def pair_copy(g, p):
        return remote(s_acc.at[g], s_in.at[g, p], s_send.at[g], s_recv.at[g, p], mate)

    def chip_copy(g, p):
        return remote(x_out.at[g], x_in.at[g, p], x_send.at[g], x_recv.at[g, p], across)

    def row_copy(g, p, i):
        return remote(t_out.at[g, i], t_in.at[g, p, i], t_send.at[g, i], t_recv.at[g, p, i], above)

    def relay(g, p):
        pair_copy(g, p).wait_recv()
        x_out[g] = s_acc[g] + s_in[g, p]
        chip_copy(g, p).start()

    def finish(g, p):
        chip_copy(g, p).wait_recv()
        u_all[g] = src[g * q:(g + 1) * q] / (x_out[g] + x_in[g, p])
        pair_copy(g, p).wait_send()
        chip_copy(g, p).wait_send()

    def send_cols(g, p):
        u = u_all[g].astype(BF16)
        for i in range(n_chunk):
            t_out[g, i] = jnp.dot(u, kern[i], preferred_element_type=F32)
            row_copy(g, p, i).start()

    def new_scale(g, p, i):
        row_copy(g, p, i).wait_recv()
        return tgt[i, g * q:(g + 1) * q] / (t_out[g, i] + t_in[g, p, i])

    def take_cols(g, p, lo, hi):
        for i in range(lo, hi):
            part = jnp.dot(new_scale(g, p, i).astype(BF16), kern_t[i], preferred_element_type=F32)
            if i == 0:
                s_acc[g] = part
            else:
                s_acc[g] += part
        if hi == n_chunk:
            pair_copy(g, 1 - p).start()
            for i in range(n_chunk):
                row_copy(g, p, i).wait_send()

    def take_last(g, p):
        for i in range(n_chunk):
            v = new_scale(g, p, i)
            v_out[g * q:(g + 1) * q, i * width:(i + 1) * width] = v
            part = _dot_t(v.astype(BF16), cost[i])
            if i == 0:
                w_acc[g] = part
            else:
                w_acc[g] += part
        for i in range(n_chunk):
            row_copy(g, p, i).wait_send()
        total = jnp.sum(u_all[g] * w_acc[g], axis=1, keepdims=True)
        spot = lax.broadcasted_iota(jnp.int32, (q, 128), 0) + g * q == lax.broadcasted_iota(jnp.int32, (q, 128), 1)
        return jnp.sum(jnp.where(spot, total, 0.0), axis=0, keepdims=True)

    def share_first(d):
        peer = lax.rem(col + d, 4)
        return remote(z_all.at[col], z_all.at[col], z_send.at[d - 1], z_recv.at[d - 1], {"col": peer})

    ones = jnp.ones((q, width), BF16)
    first = None
    for i in range(n_chunk):
        load(kern_hbm, kern, i).wait()
        part = _dot_t(ones, kern[i])
        first = part if first is None else first + part
    lanes = 128
    z_all[col] = jnp.concatenate([first[0:1, k * lanes:(k + 1) * lanes] for k in range(rows // lanes)], axis=0)
    for d in range(1, 4):
        share_first(d).start()
    for i in range(n_chunk):
        load(cost_hbm, cost, i).start()
    for i in range(n_chunk):
        kern_t[i] = kern[i].T
    src_copy.wait()
    for i in range(n_chunk):
        load_tgt(i).wait()
    for d in range(1, 4):
        share_first(d).wait()
    first_sum = (z_all[0] + z_all[1]) + (z_all[2] + z_all[3])
    for g in range(GROUPS):
        for k in range(rows // lanes):
            u_all[g, :, k * lanes:(k + 1) * lanes] = src[g * q:(g + 1) * q, k * lanes:(k + 1) * lanes] / first_sum[k:k + 1, :]

    send_cols(0, 0)
    send_cols(1, 0)
    take_cols(0, 0, 0, n_chunk)
    relay(0, 1)
    take_cols(1, 0, 0, EARLY)
    finish(0, 1)

    def sweep(step, carry):
        p = lax.rem(step, 2)
        send_cols(0, p)
        take_cols(1, 1 - p, EARLY, n_chunk)
        relay(1, p)
        take_cols(0, p, 0, EARLY)
        finish(1, p)
        send_cols(1, p)
        take_cols(0, p, EARLY, n_chunk)
        relay(0, 1 - p)
        take_cols(1, p, 0, EARLY)
        finish(0, 1 - p)
        return carry

    lax.fori_loop(1, SWEEPS - 1, sweep, 0)

    p = (SWEEPS - 1) % 2
    send_cols(0, p)
    u_out[0:q] = u_all[0]
    take_cols(1, 1 - p, EARLY, n_chunk)
    relay(1, p)
    for i in range(n_chunk):
        load(cost_hbm, cost, i).wait()
        cost[i] = kern[i] * cost[i]
    finish(1, p)
    send_cols(1, p)
    u_out[q:2 * q] = u_all[1]
    c_all[me] = jnp.broadcast_to(take_last(0, p) + take_last(1, p), (8, 128))

    def share(d):
        peer = lax.rem(me + d, 8)
        return remote(c_all.at[me], c_all.at[me], c_send.at[d - 1], c_recv.at[d - 1],
                      {"row": peer // 4, "col": lax.rem(peer, 4)})

    for d in range(1, 8):
        share(d).start()
    for d in range(1, 8):
        share(d).wait()
    grand = c_all[0]
    for j in range(1, 8):
        grand = grand + c_all[j]
    c_out[...] = grand / norm


def solution(mesh):
    row_size = mesh.shape["row"]
    col_size = mesh.shape["col"]

    def local_fn(kernel, cost_mat, src_mass, tgt_mass):
        rows, cols = kernel.shape
        batch = src_mass.shape[1]
        q = batch // GROUPS
        width = cols // CHUNKS
        norm = float(rows * row_size * cols * col_size)
        dma = pltpu.SemaphoreType.DMA
        hbm = pl.BlockSpec(memory_space=pltpu.HBM)
        vmem = pl.BlockSpec(memory_space=pltpu.VMEM)
        scratch = [
            pltpu.VMEM((CHUNKS, rows, width), BF16),
            pltpu.VMEM((CHUNKS, width, rows), BF16),
            pltpu.VMEM((CHUNKS, rows, width), BF16),
            pltpu.VMEM((batch, rows), F32),
            pltpu.VMEM((CHUNKS, batch, width), F32),
            pltpu.VMEM((GROUPS, q, rows), F32),
            pltpu.VMEM((GROUPS, q, rows), F32),
            pltpu.VMEM((GROUPS, 2, q, rows), F32),
            pltpu.VMEM((GROUPS, q, rows), F32),
            pltpu.VMEM((GROUPS, 2, q, rows), F32),
            pltpu.VMEM((GROUPS, CHUNKS, q, width), F32),
            pltpu.VMEM((GROUPS, 2, CHUNKS, q, width), F32),
            pltpu.VMEM((GROUPS, q, rows), F32),
            pltpu.VMEM((8, 8, 128), F32),
            pltpu.VMEM((4, 8, 128), F32),
            dma((CHUNKS,)), dma((CHUNKS,)), dma,
            dma((GROUPS,)), dma((GROUPS, 2)), dma((GROUPS,)), dma((GROUPS, 2)),
            dma((GROUPS, CHUNKS)), dma((GROUPS, 2, CHUNKS)), dma((7,)), dma((7,)), dma((3,)), dma((3,)),
        ]
        u_shape = jax.ShapeDtypeStruct((batch, rows), F32)
        v_shape = jax.ShapeDtypeStruct((batch, cols), F32)
        u_t, v_t, cost = pl.pallas_call(
            functools.partial(_kernel, norm),
            out_shape=(u_shape, v_shape, jax.ShapeDtypeStruct((8, 128), F32)),
            in_specs=[hbm] * 4,
            out_specs=(vmem,) * 3,
            scratch_shapes=scratch,
            compiler_params=pltpu.CompilerParams(collective_id=0, has_side_effects=True, vmem_limit_bytes=48 * 1024 * 1024),
            name="sinkhorn",
        )(kernel, cost_mat, pltpu.with_memory_space_constraint(src_mass.T, pltpu.HBM), pltpu.with_memory_space_constraint(tgt_mass.T, pltpu.HBM))
        u_t, v_t, cost = pl.pallas_call(
            _emit,
            out_shape=(u_shape, v_shape, jax.ShapeDtypeStruct((batch,), F32)),
            in_specs=[vmem] * 3,
            out_specs=(hbm, hbm, vmem),
            scratch_shapes=[dma((2,))],
            compiler_params=pltpu.CompilerParams(vmem_limit_bytes=4 * 1024 * 1024),
            name="emit",
        )(u_t, v_t, cost)
        return u_t.T, v_t.T, cost

    return jax.shard_map(local_fn, mesh=mesh, in_specs=(P("row", "col"), P("row", "col"), P("row", "prob"), P("col", "prob")), out_specs=(P("row", "prob"), P("col", "prob"), P("prob")), check_vma=False)
```

```python
import functools

import jax
import jax.numpy as jnp
from jax import lax
from jax.experimental import pallas as pl
from jax.experimental.pallas import tpu as pltpu
from jax.sharding import PartitionSpec as P

SWEEPS = 6
LOADS = 8
GROUPS = 2
STEP = 512
DIRECT = 4
TURN = 2
EARLY = 3
MIDDLE = 1
MIX = (1, 1, 1)
FIRST_MIX = ()
LAST_EARLY = 4
LAST_MIX = (2, 2, 2)
MESH = pl.DeviceIdType.MESH
F32 = jnp.float32
BF16 = jnp.bfloat16


def _dot(lhs, rhs):
    return jnp.dot(lhs, rhs, preferred_element_type=F32)


def _dot_t(lhs, rhs):
    return lax.dot_general(lhs, rhs, (((1,), (1,)), ((), ())), preferred_element_type=F32)


def _emit(u_ref, v_ref, c_ref, u_hbm, v_hbm, c_hbm, c_row, sems):
    c_row[...] = c_ref[0, 0:c_row.shape[0]]
    copies = [pltpu.make_async_copy(v_ref, v_hbm, sems.at[1]), pltpu.make_async_copy(u_ref, u_hbm, sems.at[0]),
              pltpu.make_async_copy(c_row, c_hbm, sems.at[2])]
    for copy in copies:
        copy.start()
    for copy in copies:
        copy.wait()


def _kernel(norm, kern_hbm, cost_hbm, src_hbm, tgt_hbm, u_out, v_out, c_out,
            kern, kern_t, cost, src, tgt, u_all, s_acc, lo_in, hi_in, x_out, x_in, t_out, t_in, vb_out, vb_in, w_acc, c_all, z_all,
            load_sem, tgt_sem, src_sem, lo_send, lo_recv, hi_send, hi_recv, x_send, x_recv,
            t_send, t_recv, v_send, v_recv, f_send, f_recv, c_send, c_recv, z_send, z_recv):
    row = lax.axis_index("row")
    col = lax.axis_index("col")
    core = lax.rem(col, 2)
    chip = col // 2
    mate = {"col": chip * 2 + (1 - core)}
    across = {"col": (1 - chip) * 2 + (1 - core)}
    level = {"col": (1 - chip) * 2 + core}
    above = {"row": 1 - row}
    rows, cols = kern.shape
    mid = rows // 2
    q = t_out.shape[1]
    me = row * 4 + col
    wide = cols // LOADS
    base = DIRECT * STEP
    n_last = cols // STEP

    def load(hbm, buf, i):
        part = pl.ds(i * wide, wide)
        return pltpu.make_async_copy(hbm.at[:, part], buf.at[:, part], load_sem.at[i])

    for i in range(LOADS):
        load(kern_hbm, kern, i).start()
    src_copy = pltpu.make_async_copy(src_hbm, src, src_sem)
    src_copy.start()
    tgt_copy = pltpu.make_async_copy(tgt_hbm, tgt, tgt_sem)
    tgt_copy.start()

    barrier = pltpu.get_barrier_semaphore()
    for d in range(1, 8):
        peer = lax.rem(me + d, 8)
        pl.semaphore_signal(barrier, inc=1, device_id={"row": peer // 4, "col": lax.rem(peer, 4)}, device_id_type=MESH)
    pl.semaphore_wait(barrier, 7)

    def remote(src_ref, dst_ref, send, recv, dev):
        return pltpu.make_async_remote_copy(src_ref=src_ref, dst_ref=dst_ref, send_sem=send, recv_sem=recv,
                                            device_id=dev, device_id_type=MESH)

    def turn_cols(owner, k):
        return pl.ds(pl.multiple_of(base + owner * (TURN * STEP) + k * STEP, STEP), STEP)

    def turn_slot(owner, k):
        return pl.ds(pl.multiple_of(owner * (TURN * STEP) + k * STEP, STEP), STEP)

    def line(i):
        return pl.ds(i * STEP, STEP)


    def lo_copies(g, p):
        return [remote(s_acc.at[g, :, pl.ds(0, mid)], lo_in.at[g, p, col], lo_send.at[g, j], lo_recv.at[g, p, j], dev)
                for j, dev in enumerate((across, level, mate))]

    def hi_copy(g, p):
        return remote(s_acc.at[g, :, pl.ds(mid, mid)], hi_in.at[g, p], hi_send.at[g], hi_recv.at[g, p], mate)

    def chip_copy(g, p):
        return remote(x_out.at[g], x_in.at[g, p], x_send.at[g], x_recv.at[g, p], across)

    def spread(g, p):
        hi_copy(g, p).start()
        for copy in lo_copies(g, p):
            copy.start()
        lo_in[g, p, col] = s_acc[g, :, 0:mid]

    def relay(g, p):
        hi_copy(g, p).wait_recv()
        x_out[g] = s_acc[g, :, mid:rows] + hi_in[g, p]
        chip_copy(g, p).start()

    def finish_lo(g, p):
        for copy in lo_copies(g, p):
            copy.wait_recv()
        total = (lo_in[g, p, 0] + lo_in[g, p, 1]) + (lo_in[g, p, 2] + lo_in[g, p, 3])
        u_all[g, :, 0:mid] = src[g * q:(g + 1) * q, 0:mid] / total

    def start_cols(g):
        u = u_all[g, :, 0:mid].astype(BF16)
        for i in range(n_last):
            t_out[g, :, line(i)] = _dot(u, kern[0:mid, line(i)])

    def finish_hi(g, p):
        chip_copy(g, p).wait_recv()
        u_all[g, :, mid:rows] = src[g * q:(g + 1) * q, mid:rows] / (x_out[g] + x_in[g, p])

    def settle(g, p):
        hi_copy(g, p).wait_send()
        chip_copy(g, p).wait_send()
        for copy in lo_copies(g, p):
            copy.wait_send()


    def add_cols(g, part):
        t_out[g, :, part] += _dot(u_all[g, :, mid:rows].astype(BF16), kern[mid:rows, part])

    def t_copy(g, p, i):
        part = turn_cols(1 - row, i) if i < TURN else line(i - TURN)
        return remote(t_out.at[g, :, part], t_in.at[g, p, :, part], t_send.at[g, i], t_recv.at[g, p, i], above)

    def v_copy(g, k):
        part = turn_slot(row, k)
        return remote(vb_out.at[g, :, part], vb_in.at[g, :, part], v_send.at[g, k], v_recv.at[g, k], above)

    def f_copy(g, p, i):
        return remote(t_out.at[g, :, line(i)], t_in.at[g, p, :, line(i)], f_send.at[g, i], f_recv.at[g, i], above)

    def send_ops(g, p):
        def send(i):
            add_cols(g, turn_cols(1 - row, i) if i < TURN else line(i - TURN))
            t_copy(g, p, i).start()

        def keep(k):
            add_cols(g, turn_cols(row, k))

        return [functools.partial(send, i) for i in range(TURN + DIRECT)] + [functools.partial(keep, k) for k in range(TURN)]

    def last_send_ops(g, p):
        def send(i):
            add_cols(g, line(i))
            f_copy(g, p, i).start()

        return [functools.partial(send, i) for i in range(n_last)]

    def gather(g, vb, part, first):
        got = _dot(vb, kern_t[part])
        if first:
            s_acc[g] = got
        else:
            s_acc[g] += got

    def take_ops(g, p):
        def own(k):
            t_copy(g, p, k).wait_recv()
            part = turn_cols(row, k)
            vb = (tgt[g * q:(g + 1) * q, part] / (t_out[g, :, part] + t_in[g, p, :, part])).astype(BF16)
            vb_out[g, :, turn_slot(row, k)] = vb
            v_copy(g, k).start()
            gather(g, vb, part, k == 0)

        def both(i):
            t_copy(g, p, TURN + i).wait_recv()
            part = line(i)
            vb = (tgt[g * q:(g + 1) * q, part] / (t_out[g, :, part] + t_in[g, p, :, part])).astype(BF16)
            gather(g, vb, part, False)

        def back(k):
            v_copy(g, k).wait_recv()
            gather(g, vb_in[g, :, turn_slot(1 - row, k)], turn_cols(1 - row, k), False)
            if k == TURN - 1:
                spread(g, 1 - p)

        return ([functools.partial(own, k) for k in range(TURN)] + [functools.partial(both, i) for i in range(DIRECT)]
                + [functools.partial(back, k) for k in range(TURN)])

    def last_take_ops(g, p):
        def take(i):
            f_copy(g, p, i).wait_recv()
            part = line(i)
            v = tgt[g * q:(g + 1) * q, part] / (t_out[g, :, part] + t_in[g, p, :, part])
            v_out[g * q:(g + 1) * q, part] = v
            got = _dot_t(v.astype(BF16), cost[:, part])
            if i == 0:
                w_acc[g] = got
            else:
                w_acc[g] += got

        return [functools.partial(take, i) for i in range(n_last)]

    def sent(g, p):
        for i in range(TURN + DIRECT):
            t_copy(g, p, i).wait_send()
        for k in range(TURN):
            v_copy(g, k).wait_send()

    def run(ops):
        for op in ops:
            op()

    def merge(sends, takes, mix):
        sends, takes = list(sends), list(takes)
        for count in mix:
            run(sends[:count])
            sends = sends[count:]
            run(takes[:1])
            takes = takes[1:]
        while sends or takes:
            run(sends[:1] + takes[:1])
            sends, takes = sends[1:], takes[1:]

    def cost_row(g):
        total = jnp.sum(u_all[g] * w_acc[g], axis=1, keepdims=True)
        spot = lax.broadcasted_iota(jnp.int32, (q, 128), 0) + g * q == lax.broadcasted_iota(jnp.int32, (q, 128), 1)
        return jnp.sum(jnp.where(spot, total, 0.0), axis=0, keepdims=True)


    def share_first(d):
        peer = lax.rem(col + d, 4)
        return remote(z_all.at[col], z_all.at[col], z_send.at[d - 1], z_recv.at[d - 1], {"col": peer})

    ones = jnp.ones((q, wide), BF16)
    first = None
    for i in range(LOADS):
        load(kern_hbm, kern, i).wait()
        part = _dot_t(ones, kern[:, i * wide:(i + 1) * wide])
        first = part if first is None else first + part
    lanes = 128
    z_all[col] = jnp.concatenate([first[0:1, k * lanes:(k + 1) * lanes] for k in range(rows // lanes)], axis=0)
    for d in range(1, 4):
        share_first(d).start()
    for i in range(LOADS):
        load(cost_hbm, cost, i).start()
    for i in range(LOADS):
        kern_t[i * wide:(i + 1) * wide] = kern[:, i * wide:(i + 1) * wide].T
    src_copy.wait()
    tgt_copy.wait()
    for d in range(1, 4):
        share_first(d).wait()
    first_sum = (z_all[0] + z_all[1]) + (z_all[2] + z_all[3])
    for g in range(GROUPS):
        for k in range(rows // lanes):
            u_all[g, :, k * lanes:(k + 1) * lanes] = src[g * q:(g + 1) * q, k * lanes:(k + 1) * lanes] / first_sum[k:k + 1, :]

    seen = EARLY + MIDDLE
    start_cols(0)
    run(send_ops(0, 0))
    start_cols(1)
    run(take_ops(0, 0)[:TURN])
    merge(send_ops(1, 0), take_ops(0, 0)[TURN:], FIRST_MIX)
    relay(0, 1)
    sent(0, 0)
    run(take_ops(1, 0)[:EARLY])
    finish_lo(0, 1)
    start_cols(0)
    run(take_ops(1, 0)[EARLY:seen])
    finish_hi(0, 1)

    def sweep(step, carry):
        p = lax.rem(step, 2)
        for g, pg, ph in ((0, p, 1 - p), (1, p, p)):
            h = 1 - g
            merge(send_ops(g, pg), take_ops(h, ph)[seen:], MIX)
            settle(g, pg)
            sent(h, ph)
            relay(h, 1 - ph)
            run(take_ops(g, pg)[:EARLY])
            finish_lo(h, 1 - ph)
            start_cols(h)
            run(take_ops(g, pg)[EARLY:seen])
            finish_hi(h, 1 - ph)
        return carry

    lax.fori_loop(1, SWEEPS - 1, sweep, 0)

    p = (SWEEPS - 1) % 2
    merge(last_send_ops(0, p), take_ops(1, 1 - p)[seen:], MIX)
    settle(0, p)
    u_out[0:q] = u_all[0]
    sent(1, 1 - p)
    relay(1, p)
    for i in range(LOADS):
        load(cost_hbm, cost, i).wait()
    cost[...] = kern[...] * cost[...]
    takes = last_take_ops(0, p)
    run(takes[:LAST_EARLY])
    finish_lo(1, p)
    start_cols(1)
    finish_hi(1, p)
    merge(last_send_ops(1, p), takes[LAST_EARLY:], LAST_MIX)
    settle(1, p)
    u_out[q:2 * q] = u_all[1]
    run(last_take_ops(1, p))
    for g in range(GROUPS):
        for i in range(n_last):
            f_copy(g, p, i).wait_send()
    c_all[me] = jnp.broadcast_to(cost_row(0) + cost_row(1), (8, 128))

    def share(d):
        peer = lax.rem(me + d, 8)
        return remote(c_all.at[me], c_all.at[me], c_send.at[d - 1], c_recv.at[d - 1],
                      {"row": peer // 4, "col": lax.rem(peer, 4)})

    for d in range(1, 8):
        share(d).start()
    for d in range(1, 8):
        share(d).wait()
    grand = c_all[0]
    for j in range(1, 8):
        grand = grand + c_all[j]
    c_out[...] = grand / norm


def solution(mesh):
    row_size = mesh.shape["row"]
    col_size = mesh.shape["col"]

    def local_fn(kernel, cost_mat, src_mass, tgt_mass):
        rows, cols = kernel.shape
        batch = src_mass.shape[1]
        q = batch // GROUPS
        mid = rows // 2
        norm = float(rows * row_size * cols * col_size)
        dma = pltpu.SemaphoreType.DMA
        hbm = pl.BlockSpec(memory_space=pltpu.HBM)
        vmem = pl.BlockSpec(memory_space=pltpu.VMEM)
        turn = 2 * TURN * STEP
        scratch = [
            pltpu.VMEM((rows, cols), BF16),
            pltpu.VMEM((cols, rows), BF16),
            pltpu.VMEM((rows, cols), BF16),
            pltpu.VMEM((batch, rows), F32),
            pltpu.VMEM((batch, cols), F32),
            pltpu.VMEM((GROUPS, q, rows), F32),
            pltpu.VMEM((GROUPS, q, rows), F32),
            pltpu.VMEM((GROUPS, 2, 4, q, mid), F32),
            pltpu.VMEM((GROUPS, 2, q, mid), F32),
            pltpu.VMEM((GROUPS, q, mid), F32),
            pltpu.VMEM((GROUPS, 2, q, mid), F32),
            pltpu.VMEM((GROUPS, q, cols), F32),
            pltpu.VMEM((GROUPS, 2, q, cols), F32),
            pltpu.VMEM((GROUPS, q, turn), BF16),
            pltpu.VMEM((GROUPS, q, turn), BF16),
            pltpu.VMEM((GROUPS, q, rows), F32),
            pltpu.VMEM((8, 8, 128), F32),
            pltpu.VMEM((4, 8, 128), F32),
            dma((LOADS,)), dma, dma,
            dma((GROUPS, 3)), dma((GROUPS, 2, 3)), dma((GROUPS,)), dma((GROUPS, 2)), dma((GROUPS,)), dma((GROUPS, 2)),
            dma((GROUPS, TURN + DIRECT)), dma((GROUPS, 2, TURN + DIRECT)), dma((GROUPS, TURN)), dma((GROUPS, TURN)),
            dma((GROUPS, cols // STEP)), dma((GROUPS, cols // STEP)), dma((7,)), dma((7,)), dma((3,)), dma((3,)),
        ]
        u_shape = jax.ShapeDtypeStruct((batch, rows), F32)
        v_shape = jax.ShapeDtypeStruct((batch, cols), F32)
        u_t, v_t, cost = pl.pallas_call(
            functools.partial(_kernel, norm),
            out_shape=(u_shape, v_shape, jax.ShapeDtypeStruct((8, 128), F32)),
            in_specs=[hbm] * 4,
            out_specs=(vmem,) * 3,
            scratch_shapes=scratch,
            compiler_params=pltpu.CompilerParams(collective_id=0, has_side_effects=True, vmem_limit_bytes=48 * 1024 * 1024),
            name="sinkhorn",
        )(kernel, cost_mat, pltpu.with_memory_space_constraint(src_mass.T, pltpu.HBM), pltpu.with_memory_space_constraint(tgt_mass.T, pltpu.HBM))
        u_t, v_t, cost = pl.pallas_call(
            _emit,
            out_shape=(u_shape, v_shape, jax.ShapeDtypeStruct((batch,), F32)),
            in_specs=[vmem] * 3,
            out_specs=(hbm,) * 3,
            scratch_shapes=[pltpu.VMEM((batch,), F32), dma((3,))],
            compiler_params=pltpu.CompilerParams(vmem_limit_bytes=4 * 1024 * 1024),
            name="emit",
        )(u_t, v_t, cost)
        return u_t.T, v_t.T, cost

    return jax.shard_map(local_fn, mesh=mesh, in_specs=(P("row", "col"), P("row", "col"), P("row", "prob"), P("col", "prob")), out_specs=(P("row", "prob"), P("col", "prob"), P("prob")), check_vma=False)
```

```python
import functools

import jax
import jax.numpy as jnp
from jax import lax
from jax.experimental import pallas as pl
from jax.experimental.pallas import tpu as pltpu
from jax.sharding import PartitionSpec as P

SWEEPS = 6
LOADS = 8
GROUPS = 2
STEP = 512
DIRECT = 4
TURN = 2
EARLY = 3
MIDDLE = 0
PRE = 2
LOW = 512
MIX = (2, 1, 0, 0, 0)
FIRST_MIX = ()
MESH = pl.DeviceIdType.MESH
F32 = jnp.float32
BF16 = jnp.bfloat16


def _dot(lhs, rhs):
    return jnp.dot(lhs, rhs, preferred_element_type=F32)


def _dot_t(lhs, rhs):
    return lax.dot_general(lhs, rhs, (((1,), (1,)), ((), ())), preferred_element_type=F32)


def _emit(u_ref, v_ref, c_ref, u_hbm, v_hbm, c_hbm, c_row, sems):
    c_row[...] = c_ref[0, 0:c_row.shape[0]]
    copies = [pltpu.make_async_copy(v_ref, v_hbm, sems.at[1]), pltpu.make_async_copy(u_ref, u_hbm, sems.at[0]),
              pltpu.make_async_copy(c_row, c_hbm, sems.at[2])]
    for copy in copies:
        copy.start()
    for copy in copies:
        copy.wait()


def _kernel(norm, kern_hbm, cost_hbm, src_hbm, tgt_hbm, u_out, v_out, c_out,
            kern, kern_t, cost, src, tgt, u_all, s_acc, lo_in, hi_in, x_out, x_in, t_out, t_in, vb_out, vb_in, vf_out, vf_in, w_acc, c_all, z_all,
            load_sem, tgt_sem, src_sem, lo_send, lo_recv, hi_send, hi_recv, x_send, x_recv,
            t_send, t_recv, v_send, v_recv, f_send, f_recv, c_send, c_recv, z_send, z_recv):
    row = lax.axis_index("row")
    col = lax.axis_index("col")
    core = lax.rem(col, 2)
    chip = col // 2
    mate = {"col": chip * 2 + (1 - core)}
    across = {"col": (1 - chip) * 2 + (1 - core)}
    level = {"col": (1 - chip) * 2 + core}
    above = {"row": 1 - row}
    rows, cols = kern.shape
    mid = LOW
    q = t_out.shape[1]
    me = row * 4 + col
    wide = cols // LOADS
    base = DIRECT * STEP

    def load(hbm, buf, i):
        part = pl.ds(i * wide, wide)
        return pltpu.make_async_copy(hbm.at[:, part], buf.at[:, part], load_sem.at[i])

    for i in range(LOADS):
        load(kern_hbm, kern, i).start()
    src_copy = pltpu.make_async_copy(src_hbm, src, src_sem)
    src_copy.start()
    tgt_copy = pltpu.make_async_copy(tgt_hbm, tgt, tgt_sem)
    tgt_copy.start()

    barrier = pltpu.get_barrier_semaphore()
    for d in range(1, 8):
        peer = lax.rem(me + d, 8)
        pl.semaphore_signal(barrier, inc=1, device_id={"row": peer // 4, "col": lax.rem(peer, 4)}, device_id_type=MESH)
    pl.semaphore_wait(barrier, 7)

    def remote(src_ref, dst_ref, send, recv, dev):
        return pltpu.make_async_remote_copy(src_ref=src_ref, dst_ref=dst_ref, send_sem=send, recv_sem=recv,
                                            device_id=dev, device_id_type=MESH)

    def turn_cols(owner, k):
        return pl.ds(pl.multiple_of(base + owner * (TURN * STEP) + k * STEP, STEP), STEP)

    def turn_slot(owner, k):
        return pl.ds(pl.multiple_of(owner * (TURN * STEP) + k * STEP, STEP), STEP)

    def line(i):
        return pl.ds(i * STEP, STEP)


    def lo_copies(g, p):
        return [remote(s_acc.at[g, :, pl.ds(0, mid)], lo_in.at[g, p, col], lo_send.at[g, j], lo_recv.at[g, p, j], dev)
                for j, dev in enumerate((across, level, mate))]

    def hi_copy(g, p):
        return remote(s_acc.at[g, :, pl.ds(mid, rows - mid)], hi_in.at[g, p], hi_send.at[g], hi_recv.at[g, p], mate)

    def chip_copy(g, p):
        return remote(x_out.at[g], x_in.at[g, p], x_send.at[g], x_recv.at[g, p], across)

    def spread(g, p):
        for copy in lo_copies(g, p):
            copy.start()
        lo_in[g, p, col] = s_acc[g, :, 0:mid]

    def relay(g, p):
        hi_copy(g, p).wait_recv()
        x_out[g] = s_acc[g, :, mid:rows] + hi_in[g, p]
        chip_copy(g, p).start()

    def finish_lo(g, p):
        for copy in lo_copies(g, p):
            copy.wait_recv()
        total = (lo_in[g, p, 0] + lo_in[g, p, 1]) + (lo_in[g, p, 2] + lo_in[g, p, 3])
        u_all[g, :, 0:mid] = src[g * q:(g + 1) * q, 0:mid] / total

    def start_cols(g):
        u = u_all[g, :, 0:mid].astype(BF16)
        for i in range(PRE):
            part = send_cols(i)
            t_out[g, :, part] = _dot(u, kern[0:mid, part])

    def finish_hi(g, p):
        chip_copy(g, p).wait_recv()
        u_all[g, :, mid:rows] = src[g * q:(g + 1) * q, mid:rows] / (x_out[g] + x_in[g, p])

    def settle(g, p):
        hi_copy(g, p).wait_send()
        chip_copy(g, p).wait_send()
        for copy in lo_copies(g, p):
            copy.wait_send()


    def send_cols(i):
        return turn_cols(1 - row, i) if i < TURN else line(i - TURN)

    def t_copy(g, p, i):
        part = send_cols(i)
        return remote(t_out.at[g, :, part], t_in.at[g, p, :, part], t_send.at[g, i], t_recv.at[g, p, i], above)

    def v_copy(g, k):
        part = turn_slot(row, k)
        return remote(vb_out.at[g, :, part], vb_in.at[g, :, part], v_send.at[g, k], v_recv.at[g, k], above)

    def f_copy(g, k):
        return remote(vf_out.at[g, :, turn_slot(row, k)], vf_in.at[g, :, turn_slot(row, k)], f_send.at[g, k], f_recv.at[g, k], above)

    def send_ops(g, p):
        def send(i):
            part = send_cols(i)
            if i < PRE:
                t_out[g, :, part] += _dot(u_all[g, :, mid:rows].astype(BF16), kern[mid:rows, part])
            else:
                t_out[g, :, part] = _dot(u_all[g].astype(BF16), kern[:, part])
            t_copy(g, p, i).start()

        def keep(k):
            part = turn_cols(row, k)
            t_out[g, :, part] = _dot(u_all[g].astype(BF16), kern[:, part])

        return [functools.partial(send, i) for i in range(TURN + DIRECT)] + [functools.partial(keep, k) for k in range(TURN)]

    def gather(g, vb, part, first):
        got = _dot(vb, kern_t[part])
        if first:
            s_acc[g] = got
        else:
            s_acc[g] += got

    def weigh(g, vb, part, first):
        got = _dot_t(vb, cost[:, part])
        if first:
            w_acc[g] = got
        else:
            w_acc[g] += got

    def take_ops(g, p, last=False):
        use = weigh if last else gather

        def scale(part):
            return tgt[g * q:(g + 1) * q, part] / (t_out[g, :, part] + t_in[g, p, :, part])

        def own(k):
            t_copy(g, p, k).wait_recv()
            part = turn_cols(row, k)
            v = scale(part)
            vb = v.astype(BF16)
            vb_out[g, :, turn_slot(row, k)] = vb
            v_copy(g, k).start()
            if last:
                vf_out[g, :, turn_slot(row, k)] = v
                if g == GROUPS - 1 and k == TURN - 1:
                    for h in range(GROUPS):
                        for j in range(TURN):
                            f_copy(h, j).start()
                v_out[g * q:(g + 1) * q, part] = v
            use(g, vb, part, k == 0)

        def both(i):
            t_copy(g, p, TURN + i).wait_recv()
            part = line(i)
            v = scale(part)
            if last:
                v_out[g * q:(g + 1) * q, part] = v
            use(g, v.astype(BF16), part, False)

        def back(k):
            v_copy(g, k).wait_recv()
            vb = vb_in[g, :, turn_slot(1 - row, k)]
            part = turn_cols(1 - row, k)
            if last or k < TURN - 1:
                use(g, vb, part, False)
            else:
                s_acc[g, :, mid:rows] += _dot(vb, kern_t[part, mid:rows])
                hi_copy(g, 1 - p).start()
                s_acc[g, :, 0:mid] += _dot(vb, kern_t[part, 0:mid])
                spread(g, 1 - p)

        return ([functools.partial(own, k) for k in range(TURN)] + [functools.partial(both, i) for i in range(DIRECT)]
                + [functools.partial(back, k) for k in range(TURN)])

    def sent(g, p):
        for i in range(TURN + DIRECT):
            t_copy(g, p, i).wait_send()
        for k in range(TURN):
            v_copy(g, k).wait_send()

    def run(ops):
        for op in ops:
            op()

    def merge(sends, takes, mix):
        sends, takes = list(sends), list(takes)
        for count in mix:
            run(sends[:count])
            sends = sends[count:]
            run(takes[:1])
            takes = takes[1:]
        while sends or takes:
            run(sends[:1] + takes[:1])
            sends, takes = sends[1:], takes[1:]

    def cost_row(g):
        total = jnp.sum(u_all[g] * w_acc[g], axis=1, keepdims=True)
        spot = lax.broadcasted_iota(jnp.int32, (q, 128), 0) + g * q == lax.broadcasted_iota(jnp.int32, (q, 128), 1)
        return jnp.sum(jnp.where(spot, total, 0.0), axis=0, keepdims=True)


    def share_first(d):
        peer = lax.rem(col + d, 4)
        return remote(z_all.at[col], z_all.at[col], z_send.at[d - 1], z_recv.at[d - 1], {"col": peer})

    ones = jnp.ones((q, wide), BF16)
    first = None
    for i in range(LOADS):
        load(kern_hbm, kern, i).wait()
        part = _dot_t(ones, kern[:, i * wide:(i + 1) * wide])
        first = part if first is None else first + part
    lanes = 128
    z_all[col] = jnp.concatenate([first[0:1, k * lanes:(k + 1) * lanes] for k in range(rows // lanes)], axis=0)
    for d in range(1, 4):
        share_first(d).start()
    for i in range(LOADS):
        load(cost_hbm, cost, i).start()
    for i in range(LOADS):
        kern_t[i * wide:(i + 1) * wide] = kern[:, i * wide:(i + 1) * wide].T
    src_copy.wait()
    tgt_copy.wait()
    for d in range(1, 4):
        share_first(d).wait()
    first_sum = (z_all[0] + z_all[1]) + (z_all[2] + z_all[3])
    for g in range(GROUPS):
        for k in range(rows // lanes):
            u_all[g, :, k * lanes:(k + 1) * lanes] = src[g * q:(g + 1) * q, k * lanes:(k + 1) * lanes] / first_sum[k:k + 1, :]

    seen = EARLY + MIDDLE
    start_cols(0)
    run(send_ops(0, 0))
    start_cols(1)
    run(take_ops(0, 0)[:TURN])
    merge(send_ops(1, 0), take_ops(0, 0)[TURN:], FIRST_MIX)
    relay(0, 1)
    sent(0, 0)
    run(take_ops(1, 0)[:EARLY])
    finish_lo(0, 1)
    start_cols(0)
    run(take_ops(1, 0)[EARLY:seen])
    finish_hi(0, 1)

    def sweep(step, carry):
        p = lax.rem(step, 2)
        for g, pg, ph in ((0, p, 1 - p), (1, p, p)):
            h = 1 - g
            merge(send_ops(g, pg), take_ops(h, ph)[seen:], MIX)
            settle(g, pg)
            sent(h, ph)
            relay(h, 1 - ph)
            run(take_ops(g, pg)[:EARLY])
            finish_lo(h, 1 - ph)
            start_cols(h)
            run(take_ops(g, pg)[EARLY:seen])
            finish_hi(h, 1 - ph)
        return carry

    lax.fori_loop(1, SWEEPS - 1, sweep, 0)

    p = (SWEEPS - 1) % 2
    merge(send_ops(0, p), take_ops(1, 1 - p)[seen:], MIX)
    settle(0, p)
    u_out[0:q] = u_all[0]
    sent(1, 1 - p)
    relay(1, p)
    for i in range(LOADS):
        load(cost_hbm, cost, i).wait()
    cost[...] = kern[...] * cost[...]
    takes = take_ops(0, p, True)
    run(takes[:EARLY])
    finish_lo(1, p)
    start_cols(1)
    run(takes[EARLY:seen])
    finish_hi(1, p)
    merge(send_ops(1, p), takes[seen:], MIX)
    settle(1, p)
    u_out[q:2 * q] = u_all[1]
    row_0 = cost_row(0)
    run(take_ops(1, p, True))
    c_all[me] = jnp.broadcast_to(row_0 + cost_row(1), (8, 128))

    def share(d):
        peer = lax.rem(me + d, 8)
        return remote(c_all.at[me], c_all.at[me], c_send.at[d - 1], c_recv.at[d - 1],
                      {"row": peer // 4, "col": lax.rem(peer, 4)})

    for d in range(1, 8):
        share(d).start()
    for g in range(GROUPS):
        for k in range(TURN):
            f_copy(g, k).wait()
            v_out[g * q:(g + 1) * q, turn_cols(1 - row, k)] = vf_in[g, :, turn_slot(1 - row, k)]
        sent(g, p)
    for d in range(1, 8):
        share(d).wait()
    grand = c_all[0]
    for j in range(1, 8):
        grand = grand + c_all[j]
    c_out[...] = grand / norm


def solution(mesh):
    row_size = mesh.shape["row"]
    col_size = mesh.shape["col"]

    def local_fn(kernel, cost_mat, src_mass, tgt_mass):
        rows, cols = kernel.shape
        batch = src_mass.shape[1]
        q = batch // GROUPS
        mid = LOW
        top = rows - LOW
        norm = float(rows * row_size * cols * col_size)
        dma = pltpu.SemaphoreType.DMA
        hbm = pl.BlockSpec(memory_space=pltpu.HBM)
        vmem = pl.BlockSpec(memory_space=pltpu.VMEM)
        turn = 2 * TURN * STEP
        scratch = [
            pltpu.VMEM((rows, cols), BF16),
            pltpu.VMEM((cols, rows), BF16),
            pltpu.VMEM((rows, cols), BF16),
            pltpu.VMEM((batch, rows), F32),
            pltpu.VMEM((batch, cols), F32),
            pltpu.VMEM((GROUPS, q, rows), F32),
            pltpu.VMEM((GROUPS, q, rows), F32),
            pltpu.VMEM((GROUPS, 2, 4, q, mid), F32),
            pltpu.VMEM((GROUPS, 2, q, top), F32),
            pltpu.VMEM((GROUPS, q, top), F32),
            pltpu.VMEM((GROUPS, 2, q, top), F32),
            pltpu.VMEM((GROUPS, q, cols), F32),
            pltpu.VMEM((GROUPS, 2, q, cols), F32),
            pltpu.VMEM((GROUPS, q, turn), BF16),
            pltpu.VMEM((GROUPS, q, turn), BF16),
            pltpu.VMEM((GROUPS, q, turn), F32),
            pltpu.VMEM((GROUPS, q, turn), F32),
            pltpu.VMEM((GROUPS, q, rows), F32),
            pltpu.VMEM((8, 8, 128), F32),
            pltpu.VMEM((4, 8, 128), F32),
            dma((LOADS,)), dma, dma,
            dma((GROUPS, 3)), dma((GROUPS, 2, 3)), dma((GROUPS,)), dma((GROUPS, 2)), dma((GROUPS,)), dma((GROUPS, 2)),
            dma((GROUPS, TURN + DIRECT)), dma((GROUPS, 2, TURN + DIRECT)), dma((GROUPS, TURN)), dma((GROUPS, TURN)),
            dma((GROUPS, TURN)), dma((GROUPS, TURN)), dma((7,)), dma((7,)), dma((3,)), dma((3,)),
        ]
        u_shape = jax.ShapeDtypeStruct((batch, rows), F32)
        v_shape = jax.ShapeDtypeStruct((batch, cols), F32)
        u_t, v_t, cost = pl.pallas_call(
            functools.partial(_kernel, norm),
            out_shape=(u_shape, v_shape, jax.ShapeDtypeStruct((8, 128), F32)),
            in_specs=[hbm] * 4,
            out_specs=(vmem,) * 3,
            scratch_shapes=scratch,
            compiler_params=pltpu.CompilerParams(collective_id=0, has_side_effects=True, vmem_limit_bytes=48 * 1024 * 1024),
            name="sinkhorn",
        )(kernel, cost_mat, pltpu.with_memory_space_constraint(src_mass.T, pltpu.HBM), pltpu.with_memory_space_constraint(tgt_mass.T, pltpu.HBM))
        u_t, v_t, cost = pl.pallas_call(
            _emit,
            out_shape=(u_shape, v_shape, jax.ShapeDtypeStruct((batch,), F32)),
            in_specs=[vmem] * 3,
            out_specs=(hbm,) * 3,
            scratch_shapes=[pltpu.VMEM((batch,), F32), dma((3,))],
            compiler_params=pltpu.CompilerParams(vmem_limit_bytes=4 * 1024 * 1024),
            name="emit",
        )(u_t, v_t, cost)
        return u_t.T, v_t.T, cost

    return jax.shard_map(local_fn, mesh=mesh, in_specs=(P("row", "col"), P("row", "col"), P("row", "prob"), P("col", "prob")), out_specs=(P("row", "prob"), P("col", "prob"), P("prob")), check_vma=False)
```

```python
import functools

import jax
import jax.numpy as jnp
from jax import lax
from jax.experimental import pallas as pl
from jax.experimental.pallas import tpu as pltpu
from jax.sharding import PartitionSpec as P

SWEEPS = 6
LOADS = 8
GROUPS = 2
STEP = 512
DIRECT = 4
TURN = 2
EARLY = 3
MIDDLE = 0
PRE = 2
LOW = 512
MIX = (2, 1, 0, 0, 0)
KEEP = 5
FIRST_MIX = ()
MESH = pl.DeviceIdType.MESH
F32 = jnp.float32
BF16 = jnp.bfloat16


def _dot(lhs, rhs):
    return jnp.dot(lhs, rhs, preferred_element_type=F32)


def _dot_t(lhs, rhs):
    return lax.dot_general(lhs, rhs, (((1,), (1,)), ((), ())), preferred_element_type=F32)


def _emit(u_ref, v_ref, c_ref, u_hbm, v_hbm, c_hbm, c_row, sems):
    c_row[...] = c_ref[0, 0:c_row.shape[0]]
    copies = [pltpu.make_async_copy(v_ref, v_hbm, sems.at[1]), pltpu.make_async_copy(u_ref, u_hbm, sems.at[0]),
              pltpu.make_async_copy(c_row, c_hbm, sems.at[2])]
    for copy in copies:
        copy.start()
    for copy in copies:
        copy.wait()


def _kernel(norm, kern_hbm, cost_hbm, src_hbm, tgt_hbm, u_out, v_out, c_out,
            kern, kern_t, cost, src, tgt, u_all, s_acc, lo_in, hi_in, x_out, x_in, t_out, t_in, vb_out, vb_in, vf_out, vf_in, w_acc, c_all, z_all,
            load_sem, tgt_sem, src_sem, lo_send, lo_recv, hi_send, hi_recv, x_send, x_recv,
            t_send, t_recv, v_send, v_recv, f_send, f_recv, c_send, c_recv, z_send, z_recv):
    row = lax.axis_index("row")
    col = lax.axis_index("col")
    core = lax.rem(col, 2)
    chip = col // 2
    mate = {"col": chip * 2 + (1 - core)}
    across = {"col": (1 - chip) * 2 + (1 - core)}
    level = {"col": (1 - chip) * 2 + core}
    above = {"row": 1 - row}
    rows, cols = kern.shape
    mid = LOW
    q = t_out.shape[1]
    me = row * 4 + col
    wide = cols // LOADS
    base = DIRECT * STEP

    def load(hbm, buf, i):
        part = pl.ds(i * wide, wide)
        return pltpu.make_async_copy(hbm.at[:, part], buf.at[:, part], load_sem.at[i])

    for i in range(LOADS):
        load(kern_hbm, kern, i).start()
    src_copy = pltpu.make_async_copy(src_hbm, src, src_sem)
    src_copy.start()
    tgt_copy = pltpu.make_async_copy(tgt_hbm, tgt, tgt_sem)
    tgt_copy.start()

    barrier = pltpu.get_barrier_semaphore()
    for d in range(1, 8):
        peer = lax.rem(me + d, 8)
        pl.semaphore_signal(barrier, inc=1, device_id={"row": peer // 4, "col": lax.rem(peer, 4)}, device_id_type=MESH)
    pl.semaphore_wait(barrier, 7)

    def remote(src_ref, dst_ref, send, recv, dev):
        return pltpu.make_async_remote_copy(src_ref=src_ref, dst_ref=dst_ref, send_sem=send, recv_sem=recv,
                                            device_id=dev, device_id_type=MESH)

    def turn_cols(owner, k):
        return pl.ds(pl.multiple_of(base + owner * (TURN * STEP) + k * STEP, STEP), STEP)

    def turn_slot(owner, k):
        return pl.ds(pl.multiple_of(owner * (TURN * STEP) + k * STEP, STEP), STEP)

    def line(i):
        return pl.ds(i * STEP, STEP)


    def lo_copies(g, p):
        return [remote(s_acc.at[g, :, pl.ds(0, mid)], lo_in.at[g, p, col], lo_send.at[g, j], lo_recv.at[g, p, j], dev)
                for j, dev in enumerate((across, level, mate))]

    def hi_copy(g, p):
        return remote(s_acc.at[g, :, pl.ds(mid, rows - mid)], hi_in.at[g, p], hi_send.at[g], hi_recv.at[g, p], mate)

    def chip_copy(g, p):
        return remote(x_out.at[g], x_in.at[g, p], x_send.at[g], x_recv.at[g, p], across)

    def spread(g, p):
        for copy in lo_copies(g, p):
            copy.start()
        lo_in[g, p, col] = s_acc[g, :, 0:mid]

    def relay(g, p):
        hi_copy(g, p).wait_recv()
        x_out[g] = s_acc[g, :, mid:rows] + hi_in[g, p]
        chip_copy(g, p).start()

    def finish_lo(g, p):
        for copy in lo_copies(g, p):
            copy.wait_recv()
        total = (lo_in[g, p, 0] + lo_in[g, p, 1]) + (lo_in[g, p, 2] + lo_in[g, p, 3])
        u_all[g, :, 0:mid] = src[g * q:(g + 1) * q, 0:mid] / total

    def start_cols(g):
        u = u_all[g, :, 0:mid].astype(BF16)
        for i in range(PRE):
            part = send_cols(i)
            t_out[g, :, part] = _dot(u, kern[0:mid, part])

    def finish_hi(g, p):
        chip_copy(g, p).wait_recv()
        u_all[g, :, mid:rows] = src[g * q:(g + 1) * q, mid:rows] / (x_out[g] + x_in[g, p])

    def settle(g, p):
        hi_copy(g, p).wait_send()
        chip_copy(g, p).wait_send()
        for copy in lo_copies(g, p):
            copy.wait_send()


    def send_cols(i):
        return turn_cols(1 - row, i) if i < TURN else line(i - TURN)

    def t_copy(g, p, i):
        part = send_cols(i)
        return remote(t_out.at[g, :, part], t_in.at[g, p, :, part], t_send.at[g, i], t_recv.at[g, p, i], above)

    def v_copy(g, k):
        part = turn_slot(row, k)
        return remote(vb_out.at[g, :, part], vb_in.at[g, :, part], v_send.at[g, k], v_recv.at[g, k], above)

    def f_copy(g, k):
        return remote(vf_out.at[g, :, turn_slot(row, k)], vf_in.at[g, :, turn_slot(row, k)], f_send.at[g, k], f_recv.at[g, k], above)

    def send_ops(g, p):
        def send(i):
            part = send_cols(i)
            if i < PRE:
                t_out[g, :, part] += _dot(u_all[g, :, mid:rows].astype(BF16), kern[mid:rows, part])
            else:
                t_out[g, :, part] = _dot(u_all[g].astype(BF16), kern[:, part])
            t_copy(g, p, i).start()

        def keep(k):
            part = turn_cols(row, k)
            t_out[g, :, part] = _dot(u_all[g].astype(BF16), kern[:, part])

        return [functools.partial(send, i) for i in range(TURN + DIRECT)] + [functools.partial(keep, k) for k in range(TURN)]

    def gather(g, vb, part, first):
        got = _dot(vb, kern_t[part])
        if first:
            s_acc[g] = got
        else:
            s_acc[g] += got

    def weigh(g, vb, part, first):
        got = _dot_t(vb, cost[:, part])
        if first:
            w_acc[g] = got
        else:
            w_acc[g] += got

    def take_ops(g, p, last=False):
        use = weigh if last else gather

        def scale(part):
            return tgt[g * q:(g + 1) * q, part] / (t_out[g, :, part] + t_in[g, p, :, part])

        def own(k):
            t_copy(g, p, k).wait_recv()
            part = turn_cols(row, k)
            v = scale(part)
            vb = v.astype(BF16)
            vb_out[g, :, turn_slot(row, k)] = vb
            v_copy(g, k).start()
            if last:
                vf_out[g, :, turn_slot(row, k)] = v
                if g == GROUPS - 1 and k == TURN - 1:
                    for h in range(GROUPS):
                        for j in range(TURN):
                            f_copy(h, j).start()
                v_out[g * q:(g + 1) * q, part] = v
            use(g, vb, part, k == 0)

        def both(i):
            t_copy(g, p, TURN + i).wait_recv()
            part = line(i)
            v = scale(part)
            if last:
                v_out[g * q:(g + 1) * q, part] = v
            use(g, v.astype(BF16), part, False)

        def back(k):
            v_copy(g, k).wait_recv()
            vb = vb_in[g, :, turn_slot(1 - row, k)]
            part = turn_cols(1 - row, k)
            if last or k < TURN - 1:
                use(g, vb, part, False)
            else:
                s_acc[g, :, mid:rows] += _dot(vb, kern_t[part, mid:rows])
                hi_copy(g, 1 - p).start()
                s_acc[g, :, 0:mid] += _dot(vb, kern_t[part, 0:mid])
                spread(g, 1 - p)

        return ([functools.partial(own, k) for k in range(TURN)] + [functools.partial(both, i) for i in range(DIRECT)]
                + [functools.partial(back, k) for k in range(TURN)])

    def sent(g, p):
        for i in range(TURN + DIRECT):
            t_copy(g, p, i).wait_send()
        for k in range(TURN):
            v_copy(g, k).wait_send()

    def run(ops):
        for op in ops:
            op()

    def merge(sends, takes, mix):
        sends, takes = list(sends), list(takes)
        for count in mix:
            run(sends[:count])
            sends = sends[count:]
            run(takes[:1])
            takes = takes[1:]
        while sends or takes:
            run(sends[:1] + takes[:1])
            sends, takes = sends[1:], takes[1:]

    def cost_row(g):
        total = jnp.sum(u_all[g] * w_acc[g], axis=1, keepdims=True)
        spot = lax.broadcasted_iota(jnp.int32, (q, 128), 0) + g * q == lax.broadcasted_iota(jnp.int32, (q, 128), 1)
        return jnp.sum(jnp.where(spot, total, 0.0), axis=0, keepdims=True)


    def share_first(d):
        peer = lax.rem(col + d, 4)
        return remote(z_all.at[col], z_all.at[col], z_send.at[d - 1], z_recv.at[d - 1], {"col": peer})

    ones = jnp.ones((q, wide), BF16)
    first = None
    for i in range(LOADS):
        load(kern_hbm, kern, i).wait()
        part = _dot_t(ones, kern[:, i * wide:(i + 1) * wide])
        first = part if first is None else first + part
    lanes = 128
    z_all[col] = jnp.concatenate([first[0:1, k * lanes:(k + 1) * lanes] for k in range(rows // lanes)], axis=0)
    for d in range(1, 4):
        share_first(d).start()
    for i in range(LOADS):
        load(cost_hbm, cost, i).start()
    for i in range(LOADS):
        kern_t[i * wide:(i + 1) * wide] = kern[:, i * wide:(i + 1) * wide].T
    src_copy.wait()
    tgt_copy.wait()
    for d in range(1, 4):
        share_first(d).wait()
    first_sum = (z_all[0] + z_all[1]) + (z_all[2] + z_all[3])
    for g in range(GROUPS):
        for k in range(rows // lanes):
            u_all[g, :, k * lanes:(k + 1) * lanes] = src[g * q:(g + 1) * q, k * lanes:(k + 1) * lanes] / first_sum[k:k + 1, :]

    seen = EARLY + MIDDLE
    start_cols(0)
    run(send_ops(0, 0))
    start_cols(1)
    run(take_ops(0, 0)[:TURN])
    merge(send_ops(1, 0)[:KEEP], take_ops(0, 0)[TURN:], FIRST_MIX)
    relay(0, 1)
    run(send_ops(1, 0)[KEEP:])
    run(take_ops(1, 0)[:EARLY])
    sent(0, 0)
    finish_lo(0, 1)
    start_cols(0)
    run(take_ops(1, 0)[EARLY:seen])
    finish_hi(0, 1)

    def sweep(step, carry):
        p = lax.rem(step, 2)
        for g, pg, ph in ((0, p, 1 - p), (1, p, p)):
            h = 1 - g
            merge(send_ops(g, pg)[:KEEP], take_ops(h, ph)[seen:], MIX)
            relay(h, 1 - ph)
            run(send_ops(g, pg)[KEEP:])
            settle(g, pg)
            run(take_ops(g, pg)[:EARLY])
            sent(h, ph)
            finish_lo(h, 1 - ph)
            start_cols(h)
            run(take_ops(g, pg)[EARLY:seen])
            finish_hi(h, 1 - ph)
        return carry

    lax.fori_loop(1, SWEEPS - 1, sweep, 0)

    p = (SWEEPS - 1) % 2
    merge(send_ops(0, p)[:KEEP], take_ops(1, 1 - p)[seen:], MIX)
    relay(1, p)
    run(send_ops(0, p)[KEEP:])
    settle(0, p)
    u_out[0:q] = u_all[0]
    sent(1, 1 - p)
    for i in range(LOADS):
        load(cost_hbm, cost, i).wait()
    cost[...] = kern[...] * cost[...]
    takes = take_ops(0, p, True)
    run(takes[:EARLY])
    finish_lo(1, p)
    start_cols(1)
    run(takes[EARLY:seen])
    finish_hi(1, p)
    merge(send_ops(1, p), takes[seen:], MIX)
    settle(1, p)
    u_out[q:2 * q] = u_all[1]
    row_0 = cost_row(0)
    run(take_ops(1, p, True))
    c_all[me] = jnp.broadcast_to(row_0 + cost_row(1), (8, 128))

    def share(d):
        peer = lax.rem(me + d, 8)
        return remote(c_all.at[me], c_all.at[me], c_send.at[d - 1], c_recv.at[d - 1],
                      {"row": peer // 4, "col": lax.rem(peer, 4)})

    for d in range(1, 8):
        share(d).start()
    for g in range(GROUPS):
        for k in range(TURN):
            f_copy(g, k).wait()
            v_out[g * q:(g + 1) * q, turn_cols(1 - row, k)] = vf_in[g, :, turn_slot(1 - row, k)]
        sent(g, p)
    for d in range(1, 8):
        share(d).wait()
    grand = c_all[0]
    for j in range(1, 8):
        grand = grand + c_all[j]
    c_out[...] = grand / norm


def solution(mesh):
    row_size = mesh.shape["row"]
    col_size = mesh.shape["col"]

    def local_fn(kernel, cost_mat, src_mass, tgt_mass):
        rows, cols = kernel.shape
        batch = src_mass.shape[1]
        q = batch // GROUPS
        mid = LOW
        top = rows - LOW
        norm = float(rows * row_size * cols * col_size)
        dma = pltpu.SemaphoreType.DMA
        hbm = pl.BlockSpec(memory_space=pltpu.HBM)
        vmem = pl.BlockSpec(memory_space=pltpu.VMEM)
        turn = 2 * TURN * STEP
        scratch = [
            pltpu.VMEM((rows, cols), BF16),
            pltpu.VMEM((cols, rows), BF16),
            pltpu.VMEM((rows, cols), BF16),
            pltpu.VMEM((batch, rows), F32),
            pltpu.VMEM((batch, cols), F32),
            pltpu.VMEM((GROUPS, q, rows), F32),
            pltpu.VMEM((GROUPS, q, rows), F32),
            pltpu.VMEM((GROUPS, 2, 4, q, mid), F32),
            pltpu.VMEM((GROUPS, 2, q, top), F32),
            pltpu.VMEM((GROUPS, q, top), F32),
            pltpu.VMEM((GROUPS, 2, q, top), F32),
            pltpu.VMEM((GROUPS, q, cols), F32),
            pltpu.VMEM((GROUPS, 2, q, cols), F32),
            pltpu.VMEM((GROUPS, q, turn), BF16),
            pltpu.VMEM((GROUPS, q, turn), BF16),
            pltpu.VMEM((GROUPS, q, turn), F32),
            pltpu.VMEM((GROUPS, q, turn), F32),
            pltpu.VMEM((GROUPS, q, rows), F32),
            pltpu.VMEM((8, 8, 128), F32),
            pltpu.VMEM((4, 8, 128), F32),
            dma((LOADS,)), dma, dma,
            dma((GROUPS, 3)), dma((GROUPS, 2, 3)), dma((GROUPS,)), dma((GROUPS, 2)), dma((GROUPS,)), dma((GROUPS, 2)),
            dma((GROUPS, TURN + DIRECT)), dma((GROUPS, 2, TURN + DIRECT)), dma((GROUPS, TURN)), dma((GROUPS, TURN)),
            dma((GROUPS, TURN)), dma((GROUPS, TURN)), dma((7,)), dma((7,)), dma((3,)), dma((3,)),
        ]
        u_shape = jax.ShapeDtypeStruct((batch, rows), F32)
        v_shape = jax.ShapeDtypeStruct((batch, cols), F32)
        u_t, v_t, cost = pl.pallas_call(
            functools.partial(_kernel, norm),
            out_shape=(u_shape, v_shape, jax.ShapeDtypeStruct((8, 128), F32)),
            in_specs=[hbm] * 4,
            out_specs=(vmem,) * 3,
            scratch_shapes=scratch,
            compiler_params=pltpu.CompilerParams(collective_id=0, has_side_effects=True, vmem_limit_bytes=48 * 1024 * 1024),
            name="sinkhorn",
        )(kernel, cost_mat, pltpu.with_memory_space_constraint(src_mass.T, pltpu.HBM), pltpu.with_memory_space_constraint(tgt_mass.T, pltpu.HBM))
        u_t, v_t, cost = pl.pallas_call(
            _emit,
            out_shape=(u_shape, v_shape, jax.ShapeDtypeStruct((batch,), F32)),
            in_specs=[vmem] * 3,
            out_specs=(hbm,) * 3,
            scratch_shapes=[pltpu.VMEM((batch,), F32), dma((3,))],
            compiler_params=pltpu.CompilerParams(vmem_limit_bytes=4 * 1024 * 1024),
            name="emit",
        )(u_t, v_t, cost)
        return u_t.T, v_t.T, cost

    return jax.shard_map(local_fn, mesh=mesh, in_specs=(P("row", "col"), P("row", "col"), P("row", "prob"), P("col", "prob")), out_specs=(P("row", "prob"), P("col", "prob"), P("prob")), check_vma=False)
```

```python
import functools

import jax
import jax.numpy as jnp
from jax import lax
from jax.experimental import pallas as pl
from jax.experimental.pallas import tpu as pltpu
from jax.sharding import PartitionSpec as P

SWEEPS = 6
LOADS = 8
GROUPS = 2
STEP = 512
DIRECT = 4
TURN = 2
EARLY = 3
MIDDLE = 0
PRE = 2
LOW = 512
MIX = (2, 1, 0, 0, 0)
KEEP = 5
FIRST_MIX = ()
MESH = pl.DeviceIdType.MESH
F32 = jnp.float32
BF16 = jnp.bfloat16


def _dot(lhs, rhs):
    return jnp.dot(lhs, rhs, preferred_element_type=F32)


def _dot_t(lhs, rhs):
    return lax.dot_general(lhs, rhs, (((1,), (1,)), ((), ())), preferred_element_type=F32)


def _emit(u_ref, v_ref, c_ref, u_hbm, v_hbm, c_hbm, c_row, sems):
    c_row[...] = c_ref[0, 0:c_row.shape[0]]
    copies = [pltpu.make_async_copy(v_ref, v_hbm, sems.at[1]), pltpu.make_async_copy(u_ref, u_hbm, sems.at[0]),
              pltpu.make_async_copy(c_row, c_hbm, sems.at[2])]
    for copy in copies:
        copy.start()
    for copy in copies:
        copy.wait()


def _kernel(norm, kern_hbm, cost_hbm, src_hbm, tgt_hbm, u_out, v_out, c_out,
            kern, kern_t, cost, src, tgt, u_all, s_acc, lo_in, hi_in, x_out, x_in, t_out, t_in, vb_out, vb_in, vf_out, vf_in, w_acc, c_all, z_all,
            load_sem, tgt_sem, src_sem, lo_send, lo_recv, hi_send, hi_recv, x_send, x_recv,
            t_send, t_recv, v_send, v_recv, f_send, f_recv, c_send, c_recv, z_send, z_recv):
    row = lax.axis_index("row")
    col = lax.axis_index("col")
    core = lax.rem(col, 2)
    chip = col // 2
    mate = {"col": chip * 2 + (1 - core)}
    across = {"col": (1 - chip) * 2 + (1 - core)}
    level = {"col": (1 - chip) * 2 + core}
    above = {"row": 1 - row}
    rows, cols = kern.shape
    mid = LOW
    q = t_out.shape[1]
    me = row * 4 + col
    wide = cols // LOADS
    base = DIRECT * STEP

    def load(hbm, buf, i):
        part = pl.ds(i * wide, wide)
        return pltpu.make_async_copy(hbm.at[:, part], buf.at[:, part], load_sem.at[i])

    for i in range(LOADS):
        load(kern_hbm, kern, i).start()
    src_copy = pltpu.make_async_copy(src_hbm, src, src_sem)
    src_copy.start()
    tgt_copy = pltpu.make_async_copy(tgt_hbm, tgt, tgt_sem)
    tgt_copy.start()

    barrier = pltpu.get_barrier_semaphore()
    for d in range(1, 8):
        peer = lax.rem(me + d, 8)
        pl.semaphore_signal(barrier, inc=1, device_id={"row": peer // 4, "col": lax.rem(peer, 4)}, device_id_type=MESH)
    pl.semaphore_wait(barrier, 7)

    def remote(src_ref, dst_ref, send, recv, dev):
        return pltpu.make_async_remote_copy(src_ref=src_ref, dst_ref=dst_ref, send_sem=send, recv_sem=recv,
                                            device_id=dev, device_id_type=MESH)

    def turn_cols(owner, k):
        return pl.ds(pl.multiple_of(base + owner * (TURN * STEP) + k * STEP, STEP), STEP)

    def turn_slot(owner, k):
        return pl.ds(pl.multiple_of(owner * (TURN * STEP) + k * STEP, STEP), STEP)

    def line(i):
        return pl.ds(i * STEP, STEP)


    def lo_copies(g, p):
        return [remote(s_acc.at[g, :, pl.ds(0, mid)], lo_in.at[g, p, col], lo_send.at[g, j], lo_recv.at[g, p, j], dev)
                for j, dev in enumerate((level, across, mate))]

    def hi_copy(g, p):
        return remote(s_acc.at[g, :, pl.ds(mid, rows - mid)], hi_in.at[g, p], hi_send.at[g], hi_recv.at[g, p], mate)

    def chip_copy(g, p):
        return remote(x_out.at[g], x_in.at[g, p], x_send.at[g], x_recv.at[g, p], across)

    def spread(g, p):
        for copy in lo_copies(g, p):
            copy.start()
        lo_in[g, p, col] = s_acc[g, :, 0:mid]

    def relay(g, p):
        hi_copy(g, p).wait_recv()
        x_out[g] = s_acc[g, :, mid:rows] + hi_in[g, p]
        chip_copy(g, p).start()

    def finish_lo(g, p):
        for copy in lo_copies(g, p):
            copy.wait_recv()
        total = (lo_in[g, p, 0] + lo_in[g, p, 1]) + (lo_in[g, p, 2] + lo_in[g, p, 3])
        u_all[g, :, 0:mid] = src[g * q:(g + 1) * q, 0:mid] / total

    def start_cols(g):
        u = u_all[g, :, 0:mid].astype(BF16)
        for i in range(PRE):
            part = send_cols(i)
            t_out[g, :, part] = _dot(u, kern[0:mid, part])

    def finish_hi(g, p):
        chip_copy(g, p).wait_recv()
        u_all[g, :, mid:rows] = src[g * q:(g + 1) * q, mid:rows] / (x_out[g] + x_in[g, p])

    def settle(g, p):
        hi_copy(g, p).wait_send()
        chip_copy(g, p).wait_send()
        for copy in lo_copies(g, p):
            copy.wait_send()


    def send_cols(i):
        return turn_cols(1 - row, i) if i < TURN else line(i - TURN)

    def t_copy(g, p, i):
        part = send_cols(i)
        return remote(t_out.at[g, :, part], t_in.at[g, p, :, part], t_send.at[g, i], t_recv.at[g, p, i], above)

    def v_copy(g, k):
        part = turn_slot(row, k)
        return remote(vb_out.at[g, :, part], vb_in.at[g, :, part], v_send.at[g, k], v_recv.at[g, k], above)

    def f_copy(g, k):
        return remote(vf_out.at[g, :, turn_slot(row, k)], vf_in.at[g, :, turn_slot(row, k)], f_send.at[g, k], f_recv.at[g, k], above)

    def send_ops(g, p):
        def send(i):
            part = send_cols(i)
            if i < PRE:
                t_out[g, :, part] += _dot(u_all[g, :, mid:rows].astype(BF16), kern[mid:rows, part])
            else:
                t_out[g, :, part] = _dot(u_all[g].astype(BF16), kern[:, part])
            t_copy(g, p, i).start()

        def keep(k):
            part = turn_cols(row, k)
            t_out[g, :, part] = _dot(u_all[g].astype(BF16), kern[:, part])

        return [functools.partial(send, i) for i in range(TURN + DIRECT)] + [functools.partial(keep, k) for k in range(TURN)]

    def gather(g, vb, part, first):
        got = _dot(vb, kern_t[part])
        if first:
            s_acc[g] = got
        else:
            s_acc[g] += got

    def weigh(g, vb, part, first):
        got = _dot_t(vb, cost[:, part])
        if first:
            w_acc[g] = got
        else:
            w_acc[g] += got

    def take_ops(g, p, last=False):
        use = weigh if last else gather

        def scale(part):
            return tgt[g * q:(g + 1) * q, part] / (t_out[g, :, part] + t_in[g, p, :, part])

        def own(k):
            t_copy(g, p, k).wait_recv()
            part = turn_cols(row, k)
            v = scale(part)
            vb = v.astype(BF16)
            vb_out[g, :, turn_slot(row, k)] = vb
            v_copy(g, k).start()
            if last:
                vf_out[g, :, turn_slot(row, k)] = v
                if g == GROUPS - 1 and k == TURN - 1:
                    for h in range(GROUPS):
                        for j in range(TURN):
                            f_copy(h, j).start()
                v_out[g * q:(g + 1) * q, part] = v
            use(g, vb, part, k == 0)

        def both(i):
            t_copy(g, p, TURN + i).wait_recv()
            part = line(i)
            v = scale(part)
            if last:
                v_out[g * q:(g + 1) * q, part] = v
            use(g, v.astype(BF16), part, False)

        def back(k):
            v_copy(g, k).wait_recv()
            vb = vb_in[g, :, turn_slot(1 - row, k)]
            part = turn_cols(1 - row, k)
            if last or k < TURN - 1:
                use(g, vb, part, False)
            else:
                s_acc[g, :, mid:rows] += _dot(vb, kern_t[part, mid:rows])
                hi_copy(g, 1 - p).start()
                s_acc[g, :, 0:mid] += _dot(vb, kern_t[part, 0:mid])
                spread(g, 1 - p)

        return ([functools.partial(own, k) for k in range(TURN)] + [functools.partial(both, i) for i in range(DIRECT)]
                + [functools.partial(back, k) for k in range(TURN)])

    def sent(g, p):
        for i in range(TURN + DIRECT):
            t_copy(g, p, i).wait_send()
        for k in range(TURN):
            v_copy(g, k).wait_send()

    def run(ops):
        for op in ops:
            op()

    def merge(sends, takes, mix):
        sends, takes = list(sends), list(takes)
        for count in mix:
            run(sends[:count])
            sends = sends[count:]
            run(takes[:1])
            takes = takes[1:]
        while sends or takes:
            run(sends[:1] + takes[:1])
            sends, takes = sends[1:], takes[1:]

    def cost_row(g):
        total = jnp.sum(u_all[g] * w_acc[g], axis=1, keepdims=True)
        spot = lax.broadcasted_iota(jnp.int32, (q, 128), 0) + g * q == lax.broadcasted_iota(jnp.int32, (q, 128), 1)
        return jnp.sum(jnp.where(spot, total, 0.0), axis=0, keepdims=True)


    def share_first(d):
        peer = lax.rem(col + d, 4)
        return remote(z_all.at[col], z_all.at[col], z_send.at[d - 1], z_recv.at[d - 1], {"col": peer})

    ones = jnp.ones((q, wide), BF16)
    first = None
    for i in range(LOADS):
        load(kern_hbm, kern, i).wait()
        part = _dot_t(ones, kern[:, i * wide:(i + 1) * wide])
        first = part if first is None else first + part
    lanes = 128
    z_all[col] = jnp.concatenate([first[0:1, k * lanes:(k + 1) * lanes] for k in range(rows // lanes)], axis=0)
    for d in range(1, 4):
        share_first(d).start()
    for i in range(LOADS):
        load(cost_hbm, cost, i).start()
    for i in range(LOADS):
        kern_t[i * wide:(i + 1) * wide] = kern[:, i * wide:(i + 1) * wide].T
    src_copy.wait()
    tgt_copy.wait()
    for d in range(1, 4):
        share_first(d).wait()
    first_sum = (z_all[0] + z_all[1]) + (z_all[2] + z_all[3])
    for g in range(GROUPS):
        for k in range(rows // lanes):
            u_all[g, :, k * lanes:(k + 1) * lanes] = src[g * q:(g + 1) * q, k * lanes:(k + 1) * lanes] / first_sum[k:k + 1, :]

    seen = EARLY + MIDDLE
    start_cols(0)
    run(send_ops(0, 0))
    start_cols(1)
    run(take_ops(0, 0)[:TURN])
    merge(send_ops(1, 0)[:KEEP], take_ops(0, 0)[TURN:], FIRST_MIX)
    relay(0, 1)
    run(send_ops(1, 0)[KEEP:])
    run(take_ops(1, 0)[:EARLY])
    sent(0, 0)
    finish_lo(0, 1)
    start_cols(0)
    run(take_ops(1, 0)[EARLY:seen])
    finish_hi(0, 1)

    def sweep(step, carry):
        p = lax.rem(step, 2)
        for g, pg, ph in ((0, p, 1 - p), (1, p, p)):
            h = 1 - g
            merge(send_ops(g, pg)[:KEEP], take_ops(h, ph)[seen:], MIX)
            relay(h, 1 - ph)
            run(send_ops(g, pg)[KEEP:])
            settle(g, pg)
            run(take_ops(g, pg)[:EARLY])
            sent(h, ph)
            finish_lo(h, 1 - ph)
            start_cols(h)
            run(take_ops(g, pg)[EARLY:seen])
            finish_hi(h, 1 - ph)
        return carry

    lax.fori_loop(1, SWEEPS - 1, sweep, 0)

    p = (SWEEPS - 1) % 2
    merge(send_ops(0, p)[:KEEP], take_ops(1, 1 - p)[seen:], MIX)
    relay(1, p)
    run(send_ops(0, p)[KEEP:])
    settle(0, p)
    u_out[0:q] = u_all[0]
    sent(1, 1 - p)
    for i in range(LOADS):
        load(cost_hbm, cost, i).wait()
    cost[...] = kern[...] * cost[...]
    takes = take_ops(0, p, True)
    run(takes[:TURN])
    finish_lo(1, p)
    start_cols(1)
    finish_hi(1, p)
    merge(send_ops(1, p), takes[TURN:], MIX)
    settle(1, p)
    u_out[q:2 * q] = u_all[1]
    row_0 = cost_row(0)
    run(take_ops(1, p, True))
    c_all[me] = jnp.broadcast_to(row_0 + cost_row(1), (8, 128))

    def share(d):
        peer = lax.rem(me + d, 8)
        return remote(c_all.at[me], c_all.at[me], c_send.at[d - 1], c_recv.at[d - 1],
                      {"row": peer // 4, "col": lax.rem(peer, 4)})

    for d in range(1, 8):
        share(d).start()
    for g in range(GROUPS):
        for k in range(TURN):
            f_copy(g, k).wait()
            v_out[g * q:(g + 1) * q, turn_cols(1 - row, k)] = vf_in[g, :, turn_slot(1 - row, k)]
        sent(g, p)
    for d in range(1, 8):
        share(d).wait()
    grand = c_all[0]
    for j in range(1, 8):
        grand = grand + c_all[j]
    c_out[...] = grand / norm


def solution(mesh):
    row_size = mesh.shape["row"]
    col_size = mesh.shape["col"]

    def local_fn(kernel, cost_mat, src_mass, tgt_mass):
        rows, cols = kernel.shape
        batch = src_mass.shape[1]
        q = batch // GROUPS
        mid = LOW
        top = rows - LOW
        norm = float(rows * row_size * cols * col_size)
        dma = pltpu.SemaphoreType.DMA
        hbm = pl.BlockSpec(memory_space=pltpu.HBM)
        vmem = pl.BlockSpec(memory_space=pltpu.VMEM)
        turn = 2 * TURN * STEP
        scratch = [
            pltpu.VMEM((rows, cols), BF16),
            pltpu.VMEM((cols, rows), BF16),
            pltpu.VMEM((rows, cols), BF16),
            pltpu.VMEM((batch, rows), F32),
            pltpu.VMEM((batch, cols), F32),
            pltpu.VMEM((GROUPS, q, rows), F32),
            pltpu.VMEM((GROUPS, q, rows), F32),
            pltpu.VMEM((GROUPS, 2, 4, q, mid), F32),
            pltpu.VMEM((GROUPS, 2, q, top), F32),
            pltpu.VMEM((GROUPS, q, top), F32),
            pltpu.VMEM((GROUPS, 2, q, top), F32),
            pltpu.VMEM((GROUPS, q, cols), F32),
            pltpu.VMEM((GROUPS, 2, q, cols), F32),
            pltpu.VMEM((GROUPS, q, turn), BF16),
            pltpu.VMEM((GROUPS, q, turn), BF16),
            pltpu.VMEM((GROUPS, q, turn), F32),
            pltpu.VMEM((GROUPS, q, turn), F32),
            pltpu.VMEM((GROUPS, q, rows), F32),
            pltpu.VMEM((8, 8, 128), F32),
            pltpu.VMEM((4, 8, 128), F32),
            dma((LOADS,)), dma, dma,
            dma((GROUPS, 3)), dma((GROUPS, 2, 3)), dma((GROUPS,)), dma((GROUPS, 2)), dma((GROUPS,)), dma((GROUPS, 2)),
            dma((GROUPS, TURN + DIRECT)), dma((GROUPS, 2, TURN + DIRECT)), dma((GROUPS, TURN)), dma((GROUPS, TURN)),
            dma((GROUPS, TURN)), dma((GROUPS, TURN)), dma((7,)), dma((7,)), dma((3,)), dma((3,)),
        ]
        u_shape = jax.ShapeDtypeStruct((batch, rows), F32)
        v_shape = jax.ShapeDtypeStruct((batch, cols), F32)
        u_t, v_t, cost = pl.pallas_call(
            functools.partial(_kernel, norm),
            out_shape=(u_shape, v_shape, jax.ShapeDtypeStruct((8, 128), F32)),
            in_specs=[hbm] * 4,
            out_specs=(vmem,) * 3,
            scratch_shapes=scratch,
            compiler_params=pltpu.CompilerParams(collective_id=0, has_side_effects=True, vmem_limit_bytes=48 * 1024 * 1024),
            name="sinkhorn",
        )(kernel, cost_mat, pltpu.with_memory_space_constraint(src_mass.T, pltpu.HBM), pltpu.with_memory_space_constraint(tgt_mass.T, pltpu.HBM))
        u_t, v_t, cost = pl.pallas_call(
            _emit,
            out_shape=(u_shape, v_shape, jax.ShapeDtypeStruct((batch,), F32)),
            in_specs=[vmem] * 3,
            out_specs=(hbm,) * 3,
            scratch_shapes=[pltpu.VMEM((batch,), F32), dma((3,))],
            compiler_params=pltpu.CompilerParams(vmem_limit_bytes=4 * 1024 * 1024),
            name="emit",
        )(u_t, v_t, cost)
        return u_t.T, v_t.T, cost

    return jax.shard_map(local_fn, mesh=mesh, in_specs=(P("row", "col"), P("row", "col"), P("row", "prob"), P("col", "prob")), out_specs=(P("row", "prob"), P("col", "prob"), P("prob")), check_vma=False)
```
